256 devices in a mesh: clip: 2 (over y), tm: 16 (over z), space: 4 (over x), chan: 2 (over core).
Axes of the slice: x: 4, y: 2, z: 16, core: 2. Of those that a mesh axis runs over, the one named last changes fastest.
The devices are a block of a 4x16x16 slice.
Arguments:
- features: bfloat16 [64, 16, 90, 256], P(('clip', 'tm'), 'space'), parts along dimension 0, may hold values from -700 to 700
- hidden: bfloat16 [64, 16, 90, 256], P(('clip', 'tm'), 'space'), parts along dimension 0, may hold values from -700 to 700
- cotangent: bfloat16 [64, 16, 90, 256], P(('clip', 'tm'), 'space'), parts along dimension 0, may hold values from -6 to 6
- kernel_one: bfloat16 [256, 3, 3, 3, 256], P(None, None, None, None, 'chan'), may hold values from -0.078125 to 0.078125
- kernel_two: bfloat16 [256, 3, 3, 3, 256], P(None, None, None, None, 'chan'), may hold values from -0.078125 to 0.078125
- gains: float32 [2, 256], replicated, may hold values from 0.25 to 1.75
Outputs:
- feature_grad: bfloat16 [64, 16, 90, 256], P(('clip', 'tm'), 'space', None, 'chan'), parts along dimension 0
- delta_one: float32 [512, 3, 3, 3, 256], P(('clip', 'tm', 'space'), None, None, None, 'chan'), parts along dimension 0
- delta_two: float32 [512, 3, 3, 3, 256], P(('clip', 'tm', 'space'), None, None, None, 'chan'), parts along dimension 0
- gain_grads: float32 [4, 256], P('clip', 'chan'), parts along dimension 0
The draws below stay inside these ranges and needn't reach their ends.
There are 2 independent parts, one for each index of `clip`. The reference program is written for one: setup_inputs(seed, part) draws one part's arguments, and reference() takes and returns one part's arrays. A program takes and returns all parts, laid end to end along the dimension named above; an argument that names none is the same for every part. Nothing has to cross between parts.
All inputs are finite; a program needn't handle non-finite values.
Results may differ from the reference program's by a relative error of at most 0.005.
Values may be sent and summed in bfloat16 or wider, within the bound.
A program may use at most 128 MiB of HBM per device.

```python
import math
import jax
import jax.numpy as jnp
from jax import lax

C = 256
GROUPS = 32
W = 90
FRAMES = 32
HEIGHT = 16


def field_draw(key):
    key_base, key_rows, key_chan = jax.random.split(key, 3)
    shape = (FRAMES, HEIGHT, W, C)
    row_scale = 0.2 * jnp.exp(jax.random.uniform(key_rows, (FRAMES, HEIGHT, 1, 1), jnp.float32, 0.0, math.log(10.0)))
    chan_scale = jnp.exp(jax.random.uniform(key_chan, (1, 1, 1, C), jnp.float32, 0.0, math.log(4.0)))
    position = jnp.arange(FRAMES, dtype=jnp.float32).reshape(FRAMES, 1, 1, 1) / max(FRAMES - 1, 1)
    base = jnp.clip(jax.random.normal(key_base, shape, jnp.float32), -4.0, 4.0)
    rise = jnp.exp(0.5 * math.log(3.0) * position)
    return base * row_scale * chan_scale * rise


def draw_features(key, part):
    return field_draw(jax.random.fold_in(key, 11)).astype(jnp.bfloat16)


def draw_hidden(key, part):
    return field_draw(jax.random.fold_in(key, 23)).astype(jnp.bfloat16)


def block_levels(rng, shape, cuts, least, high):
    loudness, own = 1.0, jax.random.fold_in(rng, 6)
    for dim, blocks in cuts:
        heights = jnp.exp(jax.random.uniform(jax.random.fold_in(own, dim), (blocks,), jnp.float32, least / len(cuts), high / len(cuts)))
        loudness = loudness * jnp.repeat(heights, shape[dim] // blocks).reshape([-1 if axis == dim else 1 for axis in range(len(shape))])
    return loudness


def scatter_about(stream_key, extent, deviation, bound, cuts=(), kind=jnp.bfloat16):
    entries = deviation * jax.random.normal(stream_key, extent, jnp.float32)
    if cuts:
        entries = entries * block_levels(stream_key, extent, cuts, -0.22, 0.18)
    return jnp.clip(entries, -bound, bound).astype(kind)


def setup_inputs(seed: int = 0, part: int = 0) -> dict:
    streams_of = jax.random.split(jax.random.key(seed), 7)
    part_splits = jax.random.split(jax.random.fold_in(streams_of[6], part), 7)
    features = draw_features(jax.random.fold_in(jax.random.fold_in(streams_of[6], part), 71), part)
    hidden = draw_hidden(jax.random.fold_in(jax.random.fold_in(streams_of[6], part), 71), part)
    cotangent = scatter_about(part_splits[2], (FRAMES, HEIGHT, W, C), 1.0, 6.0, ((0, 16), (1, 4)))
    kernel_one = scatter_about(streams_of[3], (C, 3, 3, 3, C), (27 * C) ** -0.5, 0.078125, ((4, 2),))
    kernel_two = scatter_about(streams_of[4], (C, 3, 3, 3, C), (27 * C) ** -0.5, 0.078125, ((4, 2),))
    gains = jnp.clip(1.0 + 0.15 * jax.random.normal(streams_of[5], (2, C), jnp.float32), 0.25, 1.75)
    return dict(features=features, hidden=hidden, cotangent=cotangent, kernel_one=kernel_one, kernel_two=kernel_two, gains=gains)


epsilon = 1e-06

def moments(field, gain, members):
    per = field.shape[3] // GROUPS
    total = lax.optimization_barrier(jnp.sum(field, axis=(0, 1, 2))).reshape(GROUPS, per)
    square = lax.optimization_barrier(jnp.sum(field * field, axis=(0, 1, 2))).reshape(GROUPS, per)
    mean = lax.optimization_barrier(jnp.sum(total, axis=1)) / members
    spread = lax.optimization_barrier(jnp.sum(square, axis=1)) / members - mean * mean
    scale = jnp.repeat(lax.rsqrt(spread + epsilon), per)
    centred = (field - jnp.repeat(mean, per)) * scale
    return (centred, centred * gain, scale)

def norm_back(upstream, centred, scaled, gain, scale, members):
    per = upstream.shape[3] // GROUPS
    gate = jax.nn.sigmoid(scaled)
    slope = upstream * gate * (1.0 + scaled * (1.0 - gate))
    plain = lax.optimization_barrier(jnp.sum(slope, axis=(0, 1, 2)))
    weighted = lax.optimization_barrier(jnp.sum(slope * centred, axis=(0, 1, 2)))
    first = jnp.repeat(lax.optimization_barrier(jnp.sum((gain * plain).reshape(-1, per), axis=1)), per) / members
    second = jnp.repeat(lax.optimization_barrier(jnp.sum((gain * weighted).reshape(-1, per), axis=1)), per) / members
    return (scale * (slope * gain - first - centred * second), weighted)

def conv_back(active, grad, kernel):
    frames, height, width, channels = active.shape
    padded = jnp.pad(grad.astype(jnp.float32), ((0, 2), (1, 1), (1, 1), (0, 0)))
    flipped = jnp.flip(jnp.transpose(kernel.astype(jnp.float32), (1, 2, 3, 4, 0)), (0, 1, 2))
    back = lax.conv_general_dilated(padded[None], flipped, (1, 1, 1), ((0, 0), (0, 0), (0, 0)), dimension_numbers=('NDHWC', 'DHWIO', 'NDHWC'), precision=lax.Precision.HIGHEST)[0]
    flat = active.reshape(-1, channels).astype(jnp.float32)
    pieces = []
    for frame_tap in range(3):
        for row_tap in range(3):
            for col_tap in range(3):
                window = padded[2 - frame_tap:2 - frame_tap + frames, 2 - row_tap:2 - row_tap + height, 2 - col_tap:2 - col_tap + width].reshape(-1, channels)
                pieces.append(lax.dot_general(flat, window, (((0,), (0,)), ((), ())), precision=lax.Precision.HIGHEST))
    delta = jnp.stack(pieces, axis=1).reshape(channels, 3, 3, 3, channels)
    return (delta, back)

def reference(features, hidden, cotangent, kernel_one, kernel_two, gains):
    members = float(FRAMES * HEIGHT * W * (C // GROUPS))
    centred_one, scaled_one, scale_one = moments(features.astype(jnp.float32), gains[0], members)
    centred_two, scaled_two, scale_two = moments(hidden.astype(jnp.float32), gains[1], members)
    active_one = (scaled_one * jax.nn.sigmoid(scaled_one)).astype(jnp.bfloat16)
    active_two = (scaled_two * jax.nn.sigmoid(scaled_two)).astype(jnp.bfloat16)
    delta_two, back_two = conv_back(active_two, cotangent, kernel_two)
    grad_two, weighted_two = norm_back(back_two, centred_two, scaled_two, gains[1], scale_two, members)
    grad_hidden = grad_two.astype(jnp.bfloat16)
    delta_one, back_one = conv_back(active_one, grad_hidden, kernel_one)
    grad_one, weighted_one = norm_back(back_one, centred_one, scaled_one, gains[0], scale_one, members)
    feature_grad = (cotangent.astype(jnp.float32) + grad_one).astype(jnp.bfloat16)
    return (feature_grad, delta_one, delta_two, jnp.stack([weighted_one, weighted_two]))
```

```python
import functools

import jax
import jax.numpy as jnp
from jax import lax
from jax.experimental import pallas as pl
from jax.experimental.pallas import tpu as pltpu
from jax.sharding import PartitionSpec as P

GROUPS = 32
EPS = 1e-06
MESH = pl.DeviceIdType.MESH
F32 = jnp.float32
BF16 = jnp.bfloat16


def padded_width(width):
    return (width + 2 + 15) // 16 * 16


def body(
    dims,
    feat_hbm, hid_hbm, cot_hbm, k1_hbm, k2_hbm, gains,
    fgrad, d1, d2, gg,
    feat, hid, cot, k1, k2,
    graw1, graw2, tmp, ext, act, act_t, perm, block_sum,
    acc, acc_in, slope, stats,
    zb_a, xb_a, zb_b, xb_b,
    xs, xa, xb, zf, zs, zr,
    in_sem, halo_s, halo_r, ar_s, ar_r, ch_s, ch_r,
    xa_s, xa_r, xb_s, xb_r, z_s, z_r,
):
    T, H, W, C, half, NT, NS = dims
    WP = padded_width(W)
    per = C // GROUPS
    share = C // (NT * NS)
    R = NT * share
    members = float(T * H * W * per * NT * NS)
    tm, sp, ch = lax.axis_index("tm"), lax.axis_index("space"), lax.axis_index("chan")
    off = pl.multiple_of(ch * half, half)
    wide = 9 * half
    K3 = 3 * half

    def at_z(d):
        return lax.rem(tm + d, NT)

    def at_x(d):
        return lax.rem(sp + d, NS)

    def signal(barrier, where):
        pl.semaphore_signal(barrier, inc=1, device_id=where, device_id_type=MESH)

    def remote(src, dst, s, r, where):
        return pltpu.make_async_remote_copy(
            src_ref=src, dst_ref=dst, send_sem=s, recv_sem=r, device_id=where, device_id_type=MESH
        )

    barrier = pltpu.get_barrier_semaphore()

    @pl.loop(1, NT)
    def _(d):
        signal(barrier, {"tm": at_z(d)})

    for d in range(1, NS):
        signal(barrier, {"space": at_x(d)})
    signal(barrier, {"chan": 1 - ch})
    for dt in (1, NT - 1):
        for ds in (1, NS - 1):
            signal(barrier, {"tm": at_z(dt), "space": at_x(ds)})

    loads = [
        pltpu.make_async_copy(src, dst, in_sem.at[i])
        for i, (src, dst) in enumerate(
            ((feat_hbm, feat), (hid_hbm, hid), (cot_hbm, cot), (k2_hbm, k2), (k1_hbm, k1))
        )
    ]
    for load in loads:
        load.start()

    tmp[...] = jnp.zeros_like(tmp)
    act[...] = jnp.zeros_like(act)
    for graw in (graw2, graw1):
        @pl.when(sp == 0)
        def _():
            graw[:, 0] = jnp.zeros((2 * T, W, half), BF16)

        @pl.when(sp == NS - 1)
        def _():
            graw[:, H + 1] = jnp.zeros((2 * T, W, half), BF16)

        @pl.when(tm == NT - 1)
        def _():
            graw[T : 2 * T] = jnp.zeros((T, H + 2, W, half), BF16)

    rows = lax.broadcasted_iota(jnp.int32, (C, C), 0)
    cols = lax.broadcasted_iota(jnp.int32, (C, C), 1)
    within = lax.rem(rows, R)
    source = within // share * (NS * share) + rows // R * share + lax.rem(within, share)
    perm[...] = jnp.where(cols == source, 1.0, 0.0).astype(BF16)
    block_sum[...] = jnp.where(rows // per == cols // per, 1.0, 0.0).astype(F32)

    def group_sum(values, width):
        return lax.dot_general(
            values, block_sum[0:width, 0:width], (((1,), (0,)), ((), ())),
            precision=lax.Precision.HIGHEST, preferred_element_type=F32,
        )

    def row_of(j):
        return j // H, lax.rem(j, H)

    for load in loads[:3]:
        load.wait()

    def stat_row(j, carry):
        t, h = row_of(j)
        out = []
        for k, ref in enumerate((feat, hid)):
            x = ref[t, h].astype(F32)
            out.append(carry[2 * k] + jnp.sum(x, axis=0, keepdims=True))
            out.append(carry[2 * k + 1] + jnp.sum(x * x, axis=0, keepdims=True))
        graw2[t, h + 1] = cot[t, h, :, pl.ds(off, half)]
        return tuple(out)

    zero_row = jnp.zeros((1, C), F32)
    sums = lax.fori_loop(0, T * H, stat_row, (zero_row,) * 4)
    for k in range(4):
        zb_a[tm, k : k + 1] = sums[k]
    pl.semaphore_wait(barrier, (NT - 1) + (NS - 1) + 1 + 4)

    def along_z(n, zb):
        @pl.loop(1, NT)
        def _(d):
            remote(zb.at[tm], zb.at[tm], ar_s.at[n, 0], ar_r.at[n, 0], {"tm": at_z(d)}).start()

    def z_to_x(n, zb, xbuf):
        every = remote(
            zb.at[0 : NT - 1], zb.at[0 : NT - 1], ar_s.at[n, 0], ar_r.at[n, 0], {"tm": at_z(1)}
        )
        every.wait_recv()
        total = lax.fori_loop(1, NT, lambda j, c: c + zb[j], zb[0])
        xbuf[sp] = total
        for d in range(1, NS):
            remote(xbuf.at[sp], xbuf.at[sp], ar_s.at[n, 1], ar_r.at[n, 1], {"space": at_x(d)}).start()

    def x_total(n, zb, xbuf):
        last = remote(
            xbuf.at[0 : NS - 1], xbuf.at[0 : NS - 1], ar_s.at[n, 1], ar_r.at[n, 1], {"space": at_x(1)}
        )
        last.wait_recv()
        total = xbuf[0]
        for j in range(1, NS):
            total = total + xbuf[j]
        return total

    def reduced_sent(n, zb, xbuf):
        remote(
            zb.at[0 : NT - 1], zb.at[0 : NT - 1], ar_s.at[n, 0], ar_r.at[n, 0], {"tm": at_z(1)}
        ).wait_send()
        remote(
            xbuf.at[0 : NS - 1], xbuf.at[0 : NS - 1], ar_s.at[n, 1], ar_r.at[n, 1], {"space": at_x(1)}
        ).wait_send()

    def halo_copies(n, graw):
        right, left = at_x(1), at_x(NS - 1)
        before = at_z(NT - 1)
        own = pl.ds(0, T)
        later = pl.ds(T, T)
        plan = (
            (graw.at[own, H], graw.at[own, 0], {"space": right}),
            (graw.at[own, 1], graw.at[own, H + 1], {"space": left}),
            (graw.at[own, pl.ds(1, H)], graw.at[later, pl.ds(1, H)], {"tm": before}),
            (graw.at[own, H], graw.at[later, 0], {"tm": before, "space": right}),
            (graw.at[own, 1], graw.at[later, H + 1], {"tm": before, "space": left}),
        )
        return [
            remote(src, dst, halo_s.at[n, i], halo_r.at[n, i], where)
            for i, (src, dst, where) in enumerate(plan)
        ]

    has_right, has_left, has_before, has_after = sp < NS - 1, sp > 0, tm > 0, tm < NT - 1
    sends = (
        has_right,
        has_left,
        has_before,
        jnp.logical_and(has_before, has_right),
        jnp.logical_and(has_before, has_left),
    )
    arrives = (
        has_left,
        has_right,
        has_after,
        jnp.logical_and(has_after, has_left),
        jnp.logical_and(has_after, has_right),
    )

    def halo_start(n, graw):
        for copy, here in zip(halo_copies(n, graw), sends):
            @pl.when(here)
            def _():
                copy.start()

    def halo_wait(n, graw, which):
        copies = halo_copies(n, graw)
        for i in which:
            @pl.when(arrives[i])
            def _():
                copies[i].wait_recv()

    def halo_sent(n, graw):
        for copy, here in zip(halo_copies(n, graw), sends):
            @pl.when(here)
            def _():
                copy.wait_send()

    def shift(graw, first, last):
        @pl.loop(first * (H + 2), last * (H + 2))
        def _(j):
            f, r = j // (H + 2), lax.rem(j, H + 2)
            tmp[8 : 8 + W] = graw[f, r].astype(F32)
            for c in range(3):
                ext[f, r, :, c * half : (c + 1) * half] = tmp[9 - c : 9 - c + WP].astype(BF16)

    def taps(f, a, b):
        return ext[f + 2 - a, 2 - b : 2 - b + H].reshape(H * WP, K3)

    def back_part(kernel, f, a, first):
        left = jnp.concatenate([taps(f, a, b) for b in range(3)], axis=1)
        right = jnp.concatenate([kernel[a * 9 + k] for k in range(9)], axis=1)
        product = lax.dot_general(left, right, (((1,), (1,)), ((), ())), preferred_element_type=F32)
        for k in range(2):
            piece = product[:, k * half : (k + 1) * half].reshape(H, WP, half)
            if first:
                acc[k, f * H : (f + 1) * H] = piece
            else:
                acc[k, f * H : (f + 1) * H] += piece

    def exchange(n):
        return remote(acc.at[1 - ch], acc_in.at[n], ch_s.at[n], ch_r.at[n], {"chan": 1 - ch})

    def delta_part(p, a):
        for b in range(3):
            right = jnp.concatenate([taps(f, a, b) for f in range(T)], axis=0)
            product = lax.dot_general(
                act_t[...], right, (((1,), (0,)), ((), ())), preferred_element_type=F32
            )
            xs[p, :, b * K3 : (b + 1) * K3] = product.astype(BF16)

    def chunk(s, part, parts):
        size = R // parts
        return pl.ds(pl.multiple_of(s * R + part * size, size), size)

    def sum_1(p):
        far = at_x(2)
        return [
            remote(
                xs.at[p, chunk(far, k, 2)], xa.at[p, k], xa_s.at[p, k], xa_r.at[p, k], {"space": at_x(d)}
            )
            for k, d in enumerate((1, NS - 1))
        ]

    def sum_2(p):
        return [
            remote(
                xs.at[p, chunk(at_x(d), 0, 1)], xb.at[p, k], xb_s.at[p, k], xb_r.at[p, k], {"space": at_x(d)}
            )
            for k, d in enumerate((1, NS - 1))
        ]

    def rs_start(p):
        for copy in sum_1(p):
            copy.start()

    def rs_pass(p):
        for k, (first, second) in enumerate(zip(sum_1(p), sum_2(p))):
            first.wait_recv()
            place = chunk(at_x((1, NS - 1)[k]), k, 2)
            xs[p, place] = (xs[p, place].astype(F32) + xa[p, k].astype(F32)).astype(BF16)
            second.start()

    def rs_z(p):
        for copy in sum_2(p):
            copy.wait_recv()
        zf[...] = xs[p, chunk(sp, 0, 1)].astype(F32) + xb[p, 0].astype(F32) + xb[p, 1].astype(F32)
        for t in range(NT):
            zs[p, t] = zf[t * share : (t + 1) * share].astype(BF16)

        @pl.loop(1, NT)
        def _(d):
            remote(zs.at[p, at_z(d)], zr.at[p, d - 1], z_s.at[p], z_r.at[p], {"tm": at_z(d)}).start()

    def z_all(p):
        return remote(zs.at[p, pl.ds(0, NT - 1)], zr.at[p], z_s.at[p], z_r.at[p], {"tm": at_z(1)})

    def rs_end(p, out, a):
        z_all(p).wait_recv()
        total = zs[p, tm].astype(F32)
        total = lax.fori_loop(0, NT - 1, lambda j, c: c + zr[p, j].astype(F32), total)
        for k in range(9):
            out[a * 9 + k] = total[:, k * half : (k + 1) * half]

    def rs_sent(p):
        for copy in sum_1(p) + sum_2(p):
            copy.wait_send()
        z_all(p).wait_send()

    def activate(ref, n):
        @pl.loop(0, T * H)
        def _(j):
            t, h = row_of(j)
            scaled = (ref[t, h].astype(F32) - stats[2 * n : 2 * n + 1]) * stats[2 * n + 1 : 2 * n + 2]
            scaled = scaled * gains[n : n + 1]
            act[j, 0:W] = (scaled * jax.nn.sigmoid(scaled)).astype(BF16)

        act_t[...] = lax.dot_general(
            perm[...], act[...].reshape(T * H * WP, C), (((1,), (1,)), ((), ())),
            preferred_element_type=F32,
        ).astype(BF16)

    def own_row(ref, k):
        return ref[k : k + 1, pl.ds(off, half)]

    def centred_row(ref, n, t, h):
        x = ref[t, h, :, pl.ds(off, half)].astype(F32)
        return (x - own_row(stats, 2 * n)) * own_row(stats, 2 * n + 1)

    def slopes(ref, n):
        exchanged = 1 - n

        def row(j, carry):
            t, h = row_of(j)
            centred = centred_row(ref, n, t, h)
            scaled = centred * own_row(gains, n)
            gate = jax.nn.sigmoid(scaled)
            upstream = acc[ch, j, 0:W] + acc_in[exchanged, j, 0:W]
            value = upstream * gate * (1.0 + scaled * (1.0 - gate))
            slope[j, 0:W] = value
            return (
                carry[0] + jnp.sum(value, axis=0, keepdims=True),
                carry[1] + jnp.sum(value * centred, axis=0, keepdims=True),
            )

        zero = jnp.zeros((1, half), F32)
        return lax.fori_loop(0, T * H, row, (zero, zero))

    def grad_rows(ref, n, totals, store):
        gain = own_row(gains, n)
        both = group_sum(totals * gain, half) * (1.0 / members)
        first, second = both[0:1], both[1:2]
        scale = own_row(stats, 2 * n + 1)
        gg[n : n + 1] = totals[1:2]

        @pl.loop(0, T * H)
        def _(j):
            t, h = row_of(j)
            centred = centred_row(ref, n, t, h)
            store(t, h, scale * (slope[j, 0:W] * gain - first - centred * second))

    def reduce_slopes(n, parts):
        for k in range(2):
            zb_b[n, tm, k : k + 1] = parts[k]
        along_z(2 - n, zb_b.at[n])

    halo_start(0, graw2)
    along_z(0, zb_a)
    z_to_x(0, zb_a, xb_a)
    halo_wait(0, graw2, range(5))
    shift(graw2, 0, 2 * T)
    loads[3].wait()
    for f in range(T):
        for a in (2, 1, 0):
            back_part(k2, f, a, a == 2)
    exchange(0).start()
    totals = group_sum(x_total(0, zb_a, xb_a), C) * (1.0 / members)
    for n in range(2):
        mean = totals[2 * n : 2 * n + 1]
        spread = totals[2 * n + 1 : 2 * n + 2] - mean * mean
        stats[2 * n : 2 * n + 1] = mean
        stats[2 * n + 1 : 2 * n + 2] = lax.rsqrt(spread + EPS)
    exchange(0).wait_recv()
    reduce_slopes(1, slopes(hid, 1))
    activate(hid, 1)
    for p in range(3):
        delta_part(p, 2 - p)
        rs_start(p)
    z_to_x(1, zb_b.at[1], xb_b.at[1])
    rs_pass(0)
    totals_two = x_total(1, zb_b.at[1], xb_b.at[1])

    def store_hidden(t, h, value):
        graw1[t, h + 1] = value.astype(BF16)

    grad_rows(hid, 1, totals_two, store_hidden)

    halo_start(1, graw1)
    rs_pass(1)
    rs_pass(2)
    activate(feat, 0)
    halo_wait(1, graw1, (0, 1))
    shift(graw1, 0, T)
    delta_part(3, 2)
    rs_start(3)
    loads[4].wait()
    exchange(0).wait_send()
    for f in range(T):
        for a in (2, 1):
            if f + 2 - a < T:
                back_part(k1, f, a, a == 2)
    rs_z(0)
    halo_wait(1, graw1, (2, 3, 4))
    shift(graw1, T, 2 * T)
    for f in range(T):
        for a in (1, 0):
            if f + 2 - a >= T:
                back_part(k1, f, a, False)
    exchange(1).start()
    for p in (4, 5):
        delta_part(p, 5 - p)
        rs_start(p)
    exchange(1).wait_recv()
    reduce_slopes(0, slopes(feat, 0))
    rs_pass(3)
    rs_z(1)
    rs_z(2)
    rs_pass(4)
    rs_pass(5)
    z_to_x(2, zb_b.at[0], xb_b.at[0])
    rs_z(3)
    totals_one = x_total(2, zb_b.at[0], xb_b.at[0])

    def store_feature(t, h, value):
        base = cot[t, h, :, pl.ds(off, half)].astype(F32)
        fgrad[t, h] = (base + value).astype(BF16)

    grad_rows(feat, 0, totals_one, store_feature)
    rs_z(4)
    rs_z(5)
    for p in range(6):
        rs_end(p, (d2, d1)[p // 3], 2 - p % 3)

    halo_sent(0, graw2)
    halo_sent(1, graw1)
    reduced_sent(0, zb_a, xb_a)
    reduced_sent(1, zb_b.at[1], xb_b.at[1])
    reduced_sent(2, zb_b.at[0], xb_b.at[0])
    exchange(1).wait_send()
    for p in range(6):
        rs_sent(p)


def shards(features, hidden, cotangent, kernel_one, kernel_two, gains):
    T, H, W, C = features.shape
    half = kernel_one.shape[4]
    NT, NS = lax.axis_size("tm"), lax.axis_size("space")
    share = C // (NT * NS)
    R = NT * share
    WP = padded_width(W)
    wide = 9 * half

    def by_tap(kernel):
        return jnp.transpose(kernel, (1, 2, 3, 0, 4)).reshape(27, C, half)

    vmem = pl.BlockSpec(memory_space=pltpu.VMEM)
    hbm = pl.BlockSpec(memory_space=pl.ANY)
    DMA = pltpu.SemaphoreType.DMA
    call = pl.pallas_call(
        functools.partial(body, (T, H, W, C, half, NT, NS)),
        out_shape=(
            jax.ShapeDtypeStruct((T, H, W, half), BF16),
            jax.ShapeDtypeStruct((27, share, half), F32),
            jax.ShapeDtypeStruct((27, share, half), F32),
            jax.ShapeDtypeStruct((2, half), F32),
        ),
        in_specs=[hbm] * 5 + [vmem],
        out_specs=(vmem,) * 4,
        scratch_shapes=[
            pltpu.VMEM((T, H, W, C), BF16),
            pltpu.VMEM((T, H, W, C), BF16),
            pltpu.VMEM((T, H, W, C), BF16),
            pltpu.VMEM((27, C, half), BF16),
            pltpu.VMEM((27, C, half), BF16),
            pltpu.VMEM((2 * T, H + 2, W, half), BF16),
            pltpu.VMEM((2 * T, H + 2, W, half), BF16),
            pltpu.VMEM((WP + 16, half), F32),
            pltpu.VMEM((2 * T, H + 2, WP, 3 * half), BF16),
            pltpu.VMEM((T * H, WP, C), BF16),
            pltpu.VMEM((C, T * H * WP), BF16),
            pltpu.VMEM((C, C), BF16),
            pltpu.VMEM((C, C), F32),
            pltpu.VMEM((2, T * H, WP, half), F32),
            pltpu.VMEM((2, T * H, WP, half), F32),
            pltpu.VMEM((T * H, WP, half), F32),
            pltpu.VMEM((8, C), F32),
            pltpu.VMEM((NT, 4, C), F32),
            pltpu.VMEM((NS, 4, C), F32),
            pltpu.VMEM((2, NT, 2, half), F32),
            pltpu.VMEM((2, NS, 2, half), F32),
            pltpu.VMEM((6, C, wide), BF16),
            pltpu.VMEM((6, 2, R // 2, wide), BF16),
            pltpu.VMEM((6, 2, R, wide), BF16),
            pltpu.VMEM((R, wide), F32),
            pltpu.VMEM((6, NT, share, wide), BF16),
            pltpu.VMEM((6, NT - 1, share, wide), BF16),
            DMA((5,)),
            DMA((2, 5)),
            DMA((2, 5)),
            DMA((3, 2)),
            DMA((3, 2)),
            DMA((2,)),
            DMA((2,)),
            DMA((6, 2)),
            DMA((6, 2)),
            DMA((6, 2)),
            DMA((6, 2)),
            DMA((6,)),
            DMA((6,)),
        ],
        compiler_params=pltpu.CompilerParams(
            collective_id=0, has_side_effects=True, vmem_limit_bytes=60 * 1024 * 1024
        ),
        name="block_back",
    )
    fgrad, d1, d2, gg = call(
        features, hidden, cotangent, by_tap(kernel_one), by_tap(kernel_two), gains
    )

    def by_channel(delta):
        return jnp.transpose(delta.reshape(3, 3, 3, share, half), (3, 0, 1, 2, 4))

    return (fgrad, by_channel(d1), by_channel(d2), gg)


def solution(mesh):
    placed = (
        P(("clip", "tm"), "space", None, None),
        P(("clip", "tm"), "space", None, None),
        P(("clip", "tm"), "space", None, None),
        P(None, None, None, None, "chan"),
        P(None, None, None, None, "chan"),
        P(),
    )
    return jax.shard_map(
        shards,
        mesh=mesh,
        in_specs=placed,
        out_specs=(
            P(("clip", "tm"), "space", None, "chan"),
            P(("clip", "tm", "space"), None, None, None, "chan"),
            P(("clip", "tm", "space"), None, None, None, "chan"),
            P("clip", "chan"),
        ),
        check_vma=False,
    )
```

```python
import functools

import jax
import jax.numpy as jnp
from jax import lax
from jax.experimental import pallas as pl
from jax.experimental.pallas import tpu as pltpu
from jax.sharding import PartitionSpec as P

GROUPS = 32
EPS = 1e-06
MESH = pl.DeviceIdType.MESH
F32 = jnp.float32
BF16 = jnp.bfloat16


def padded_width(width):
    return (width + 2 + 15) // 16 * 16


def body(
    dims,
    feat_hbm, hid_hbm, cot_hbm, k1_hbm, k2_hbm, gains,
    fgrad, d1, d2, gg,
    feat_n, hid_n, cot_n, feat, hid, k1, k2,
    graw2, graw1, turn, turn_half, tmp, ext, act, act_t, perm, block_sum, spread_sum,
    acc, acc_in, slope, stats,
    zb_a, xb_a, zb_b, xb_b,
    xs, xa, xb, zf, zk, zs, za, zc, zr,
    in_sem, halo_s, halo_r, ar_s, ar_r, ch_s, ch_r,
    xa_s, xa_r, xb_s, xb_r, za_s, za_r, z_s, z_r,
):
    T, H, W, C, half, NT, NS = dims
    WP = padded_width(W)
    per = C // GROUPS
    share = C // (NT * NS)
    R = NT * share
    members = float(T * H * W * per * NT * NS)
    tm, sp, ch = lax.axis_index("tm"), lax.axis_index("space"), lax.axis_index("chan")
    off = pl.multiple_of(ch * half, half)
    wide = 9 * half
    K3 = 3 * half

    def at_z(d):
        return lax.rem(tm + d, NT)

    def at_x(d):
        return lax.rem(sp + d, NS)

    def signal(barrier, where):
        pl.semaphore_signal(barrier, inc=1, device_id=where, device_id_type=MESH)

    def remote(src, dst, s, r, where):
        return pltpu.make_async_remote_copy(
            src_ref=src, dst_ref=dst, send_sem=s, recv_sem=r, device_id=where, device_id_type=MESH
        )

    barrier = pltpu.get_barrier_semaphore()

    @pl.loop(1, NT)
    def _(d):
        signal(barrier, {"tm": at_z(d)})

    for d in range(1, NS):
        signal(barrier, {"space": at_x(d)})
    signal(barrier, {"chan": 1 - ch})
    for dt in (1, NT - 1):
        for ds in (1, NS - 1):
            signal(barrier, {"tm": at_z(dt), "space": at_x(ds)})

    loads = [
        pltpu.make_async_copy(src, dst, in_sem.at[i])
        for i, (src, dst) in enumerate(
            ((feat_hbm, feat_n), (hid_hbm, hid_n), (cot_hbm, cot_n), (k2_hbm, k2), (k1_hbm, k1))
        )
    ]
    for load in loads:
        load.start()

    def group_sum(values, width):
        return lax.dot_general(
            values, block_sum[0:width, 0:width], (((1,), (0,)), ((), ())),
            precision=lax.Precision.HIGHEST, preferred_element_type=F32,
        )

    def row_of(j):
        return j // H, lax.rem(j, H)

    for load in loads[:3]:
        load.wait()

    rows = lax.broadcasted_iota(jnp.int32, (C, half), 0)
    cols = lax.broadcasted_iota(jnp.int32, (C, half), 1)
    spread_sum[...] = jnp.where(rows // per == cols, 1.0, 0.0).astype(F32)
    strip = W // 9 if W % 9 == 0 else 1

    def stat_strip(j, carry):
        t, w = j // (W // strip), lax.rem(j, W // strip) * strip
        out = []
        for k, ref in enumerate((feat_n, hid_n)):
            x = ref[t, pl.ds(w, strip)].astype(F32)
            out.append(carry[2 * k] + jnp.sum(x, axis=0))
            out.append(carry[2 * k + 1] + jnp.sum(x * x, axis=0))
        return tuple(out)

    sums = lax.fori_loop(0, T * (W // strip), stat_strip, (jnp.zeros((H, C), F32),) * 4)
    sums = jnp.concatenate([jnp.sum(x, axis=0, keepdims=True) for x in sums], axis=0)
    zb_a[tm] = lax.dot_general(
        sums, spread_sum[...], (((1,), (0,)), ((), ())),
        precision=lax.Precision.HIGHEST, preferred_element_type=F32,
    )
    for t in range(T):
        turn_half[t] = cot_n[t, :, :, pl.ds(off, half)].astype(F32)
        for h in range(H):
            graw2[t, h + 1] = turn_half[t, :, h, :].astype(BF16)
    pl.semaphore_wait(barrier, (NT - 1) + (NS - 1) + 1 + 4)

    def along_z(n, zb):
        @pl.loop(0, NT - 1)
        def _(k):
            step = (k + 1) // 2
            d = NT // 2 + jnp.where(lax.rem(k, 2) == 0, step, -step)
            remote(zb.at[tm], zb.at[tm], ar_s.at[n, 0], ar_r.at[n, 0], {"tm": at_z(d)}).start()

    def z_to_x(n, zb, xbuf):
        every = remote(
            zb.at[0 : NT - 1], zb.at[0 : NT - 1], ar_s.at[n, 0], ar_r.at[n, 0], {"tm": at_z(1)}
        )
        every.wait_recv()
        total = lax.fori_loop(1, NT, lambda j, c: c + zb[j], zb[0])
        xbuf[sp] = total
        for d in range(1, NS):
            remote(xbuf.at[sp], xbuf.at[sp], ar_s.at[n, 1], ar_r.at[n, 1], {"space": at_x(d)}).start()

    def x_total(n, zb, xbuf):
        last = remote(
            xbuf.at[0 : NS - 1], xbuf.at[0 : NS - 1], ar_s.at[n, 1], ar_r.at[n, 1], {"space": at_x(1)}
        )
        last.wait_recv()
        total = xbuf[0]
        for j in range(1, NS):
            total = total + xbuf[j]
        return total

    def reduced_sent(n, zb, xbuf):
        remote(
            zb.at[0 : NT - 1], zb.at[0 : NT - 1], ar_s.at[n, 0], ar_r.at[n, 0], {"tm": at_z(1)}
        ).wait_send()
        remote(
            xbuf.at[0 : NS - 1], xbuf.at[0 : NS - 1], ar_s.at[n, 1], ar_r.at[n, 1], {"space": at_x(1)}
        ).wait_send()

    def halo_copies(n, graw):
        right, left = at_x(1), at_x(NS - 1)
        before = at_z(NT - 1)
        own = pl.ds(0, T)
        later = pl.ds(T, T)
        plan = (
            (graw.at[own, H], graw.at[own, 0], {"space": right}),
            (graw.at[own, 1], graw.at[own, H + 1], {"space": left}),
            (graw.at[own, pl.ds(1, H)], graw.at[later, pl.ds(1, H)], {"tm": before}),
            (graw.at[own, H], graw.at[later, 0], {"tm": before, "space": right}),
            (graw.at[own, 1], graw.at[later, H + 1], {"tm": before, "space": left}),
        )
        return [
            remote(src, dst, halo_s.at[n, i], halo_r.at[n, i], where)
            for i, (src, dst, where) in enumerate(plan)
        ]

    has_right, has_left, has_before, has_after = sp < NS - 1, sp > 0, tm > 0, tm < NT - 1
    sends = (
        has_right,
        has_left,
        has_before,
        jnp.logical_and(has_before, has_right),
        jnp.logical_and(has_before, has_left),
    )
    arrives = (
        has_left,
        has_right,
        has_after,
        jnp.logical_and(has_after, has_left),
        jnp.logical_and(has_after, has_right),
    )

    def halo_start(n, graw):
        for copy, here in zip(halo_copies(n, graw), sends):
            @pl.when(here)
            def _():
                copy.start()

    def halo_wait(n, graw, which):
        copies = halo_copies(n, graw)
        for i in which:
            @pl.when(arrives[i])
            def _():
                copies[i].wait_recv()

    def halo_sent(n, graw):
        for copy, here in zip(halo_copies(n, graw), sends):
            @pl.when(here)
            def _():
                copy.wait_send()

    def place_shifted(f, r, values):
        tmp[8 : 8 + W] = values
        for c in range(3):
            ext[f, r, :, c * half : (c + 1) * half] = tmp[9 - c : 9 - c + WP].astype(BF16)

    def shift(graw, first, last):
        @pl.loop(first * (H + 2), last * (H + 2))
        def _(j):
            f, r = j // (H + 2), lax.rem(j, H + 2)
            place_shifted(f, r, graw[f, r].astype(F32))

    def taps(f, a, b):
        return ext[f + 2 - a, 2 - b : 2 - b + H].reshape(H * WP, K3)

    def back_part(kernel, f, a, first):
        left = jnp.concatenate([taps(f, a, b) for b in range(3)], axis=1)
        right = jnp.concatenate([kernel[a * 9 + k] for k in range(9)], axis=1)
        product = lax.dot_general(left, right, (((1,), (1,)), ((), ())), preferred_element_type=F32)
        for k in range(2):
            piece = product[:, k * half : (k + 1) * half].reshape(H, WP, half)
            if first:
                acc[k, f * H : (f + 1) * H] = piece
            else:
                acc[k, f * H : (f + 1) * H] += piece

    def exchange(n):
        return remote(acc.at[1 - ch], acc_in.at[n], ch_s.at[n], ch_r.at[n], {"chan": 1 - ch})

    def delta_part(p, a):
        for b in range(3):
            right = jnp.concatenate([taps(f, a, b) for f in range(T)], axis=0)
            product = lax.dot_general(
                act_t[...], right, (((1,), (0,)), ((), ())), preferred_element_type=F32
            )
            xs[p, :, b * K3 : (b + 1) * K3] = product.astype(BF16)

    def chunk(s, part, parts):
        size = R // parts
        return pl.ds(pl.multiple_of(s * R + part * size, size), size)

    def sum_1(p):
        far = at_x(2)
        return [
            remote(
                xs.at[p, chunk(far, k, 2)], xa.at[p, k], xa_s.at[p, k], xa_r.at[p, k], {"space": at_x(d)}
            )
            for k, d in enumerate((1, NS - 1))
        ]

    def sum_2(p):
        return [
            remote(
                xs.at[p, chunk(at_x(d), 0, 1)], xb.at[p, k], xb_s.at[p, k], xb_r.at[p, k], {"space": at_x(d)}
            )
            for k, d in enumerate((1, NS - 1))
        ]

    def rs_start(p):
        for copy in sum_1(p):
            copy.start()

    def rs_pass(p):
        for k, (first, second) in enumerate(zip(sum_1(p), sum_2(p))):
            first.wait_recv()
            place = chunk(at_x((1, NS - 1)[k]), k, 2)
            xs[p, place] = (xs[p, place].astype(F32) + xa[p, k].astype(F32)).astype(BF16)
            second.start()

    pairs = NT // 2
    parity = lax.rem(tm, 2)
    place = tm // 2
    mate = tm + 1 - 2 * parity

    def to_mate(p):
        return remote(zs.at[p, 1 - parity], za.at[p], za_s.at[p], za_r.at[p], {"tm": mate})

    def rs_z1(p):
        for copy in sum_2(p):
            copy.wait_recv()
        zf[...] = xs[p, chunk(sp, 0, 1)].astype(F32) + xb[p, 0].astype(F32) + xb[p, 1].astype(F32)
        for t in range(NT):
            rows = zf[t * share : (t + 1) * share]
            zk[p, t % 2, t // 2] = rows
            zs[p, t % 2, t // 2] = rows.astype(BF16)
        to_mate(p).start()

    def rs_z2(p):
        to_mate(p).wait_recv()

        @pl.loop(0, pairs)
        def _(j):
            both = zk[p, parity, j] + za[p, j].astype(F32)
            zk[p, parity, j] = both
            zc[p, j] = both.astype(BF16)

        @pl.loop(1, pairs)
        def _(d):
            to = lax.rem(place + d, pairs)
            remote(zc.at[p, to], zr.at[p, d - 1], z_s.at[p], z_r.at[p], {"tm": 2 * to + parity}).start()

    def z_all(p):
        return remote(zc.at[p, pl.ds(0, pairs - 1)], zr.at[p], z_s.at[p], z_r.at[p], {"tm": mate})

    def rs_end(p, out, a):
        z_all(p).wait_recv()
        total = zk[p, parity, place]
        for j in range(pairs - 1):
            total = total + zr[p, j].astype(F32)
        for k in range(9):
            out[a * 9 + k] = total[:, k * half : (k + 1) * half]

    def rs_sent(p):
        for copy in sum_1(p) + sum_2(p):
            copy.wait_send()
        to_mate(p).wait_send()
        z_all(p).wait_send()

    def activate(ref, n):
        @pl.loop(0, T * H)
        def _(j):
            t, h = row_of(j)
            scaled = (ref[t, h].astype(F32) - stats[2 * n : 2 * n + 1]) * stats[2 * n + 1 : 2 * n + 2]
            scaled = scaled * gains[n : n + 1]
            act[j, 0:W] = (scaled * jax.nn.sigmoid(scaled)).astype(BF16)

        act_t[...] = lax.dot_general(
            perm[...], act[...].reshape(T * H * WP, C), (((1,), (1,)), ((), ())),
            preferred_element_type=F32,
        ).astype(BF16)

    def own_row(ref, k):
        return ref[k : k + 1, pl.ds(off, half)]

    def centred_row(ref, n, t, h):
        x = ref[t, h, :, pl.ds(off, half)].astype(F32)
        return (x - own_row(stats, 2 * n)) * own_row(stats, 2 * n + 1)

    def slopes(ref, n):
        exchanged = 1 - n

        def row(j, carry):
            t, h = row_of(j)
            centred = centred_row(ref, n, t, h)
            scaled = centred * own_row(gains, n)
            gate = jax.nn.sigmoid(scaled)
            upstream = acc[ch, j, 0:W] + acc_in[exchanged, j, 0:W]
            value = upstream * gate * (1.0 + scaled * (1.0 - gate))
            slope[j, 0:W] = value
            return (
                carry[0] + jnp.sum(value, axis=0, keepdims=True),
                carry[1] + jnp.sum(value * centred, axis=0, keepdims=True),
            )

        zero = jnp.zeros((1, half), F32)
        return lax.fori_loop(0, T * H, row, (zero, zero))

    def norm_terms(n, totals):
        both = group_sum(totals * own_row(gains, n), half) * (1.0 / members)
        gg[n : n + 1] = totals[1:2]
        return both[0:1], both[1:2]

    def grad_row(ref, n, t, h, terms):
        first, second = terms
        centred = centred_row(ref, n, t, h)
        inner = slope[t * H + h, 0:W] * own_row(gains, n) - first - centred * second
        return own_row(stats, 2 * n + 1) * inner

    def hidden_rows(totals):
        terms = norm_terms(1, totals)

        @pl.loop(0, T * H)
        def _(j):
            t, h = row_of(j)
            graw1[t, h + 1] = grad_row(hid, 1, t, h, terms).astype(BF16)

    def feature_rows(totals):
        terms = norm_terms(0, totals)

        @pl.loop(0, T)
        def _(t):
            for h in range(H):
                base = graw2[t, h + 1].astype(F32)
                turn_half[t, :, h, :] = base + grad_row(feat, 0, t, h, terms)
            fgrad[t] = turn_half[t].astype(BF16)

    def by_rows(source, target):
        @pl.loop(0, T)
        def _(t):
            turn[...] = source[t].astype(F32)
            for h in range(H):
                target[t, h] = turn[:, h, :].astype(BF16)

    def reduce_slopes(n, parts):
        for k in range(2):
            zb_b[n, tm, k : k + 1] = parts[k]
        along_z(2 - n, zb_b.at[n])

    along_z(0, zb_a)
    halo_start(0, graw2)
    tmp[...] = jnp.zeros_like(tmp)
    act[...] = jnp.zeros_like(act)
    for graw in (graw2, graw1):
        @pl.when(sp == 0)
        def _():
            graw[:, 0] = jnp.zeros((2 * T, W, half), BF16)

        @pl.when(sp == NS - 1)
        def _():
            graw[:, H + 1] = jnp.zeros((2 * T, W, half), BF16)

        @pl.when(tm == NT - 1)
        def _():
            graw[T : 2 * T] = jnp.zeros((T, H + 2, W, half), BF16)

    rows = lax.broadcasted_iota(jnp.int32, (C, C), 0)
    cols = lax.broadcasted_iota(jnp.int32, (C, C), 1)
    within = lax.rem(rows, R)
    source = within // share * (NS * share) + rows // R * share + lax.rem(within, share)
    perm[...] = jnp.where(cols == source, 1.0, 0.0).astype(BF16)
    block_sum[...] = jnp.where(rows // per == cols // per, 1.0, 0.0).astype(F32)
    by_rows(hid_n, hid)
    by_rows(feat_n, feat)
    halo_wait(0, graw2, range(5))
    shift(graw2, 0, 2 * T)
    loads[3].wait()
    for f in range(T):
        for a in (2, 1, 0):
            back_part(k2, f, a, a == 2)
    exchange(0).start()
    z_to_x(0, zb_a, xb_a)
    totals = lax.dot_general(
        x_total(0, zb_a, xb_a), spread_sum[...], (((1,), (1,)), ((), ())),
        precision=lax.Precision.HIGHEST, preferred_element_type=F32,
    ) * (1.0 / members)
    for n in range(2):
        mean = totals[2 * n : 2 * n + 1]
        spread = totals[2 * n + 1 : 2 * n + 2] - mean * mean
        stats[2 * n : 2 * n + 1] = mean
        stats[2 * n + 1 : 2 * n + 2] = lax.rsqrt(spread + EPS)
    exchange(0).wait_recv()
    reduce_slopes(1, slopes(hid, 1))
    activate(hid, 1)
    for p in range(3):
        delta_part(p, 2 - p)
        rs_start(p)
    activate(feat, 0)
    z_to_x(1, zb_b.at[1], xb_b.at[1])
    rs_pass(0)
    totals_two = x_total(1, zb_b.at[1], xb_b.at[1])

    hidden_rows(totals_two)
    halo_start(1, graw1)
    rs_pass(1)
    rs_pass(2)
    halo_wait(1, graw1, (0, 1))
    shift(graw1, 0, T)
    delta_part(3, 2)
    rs_start(3)
    loads[4].wait()
    exchange(0).wait_send()
    for f in range(T):
        for a in (2, 1):
            if f + 2 - a < T:
                back_part(k1, f, a, a == 2)
    rs_z1(0)
    halo_wait(1, graw1, (2, 3, 4))
    shift(graw1, T, 2 * T)
    for p in range(4, 6):
        delta_part(p, 5 - p)
        rs_start(p)
    rs_z1(1)
    rs_pass(3)
    for f in range(T):
        for a in (1, 0):
            if f + 2 - a >= T:
                back_part(k1, f, a, False)
    exchange(1).start()
    rs_z1(2)
    rs_z2(0)
    rs_pass(4)
    exchange(1).wait_recv()
    reduce_slopes(0, slopes(feat, 0))
    rs_pass(5)
    rs_z2(1)
    rs_z2(2)
    rs_z1(3)
    z_to_x(2, zb_b.at[0], xb_b.at[0])
    rs_z1(4)
    rs_z2(3)
    feature_rows(x_total(2, zb_b.at[0], xb_b.at[0]))
    rs_z1(5)
    rs_z2(4)
    rs_z2(5)
    for p in range(6):
        rs_end(p, (d2, d1)[p // 3], 2 - p % 3)

    halo_sent(0, graw2)
    halo_sent(1, graw1)
    reduced_sent(0, zb_a, xb_a)
    reduced_sent(1, zb_b.at[1], xb_b.at[1])
    reduced_sent(2, zb_b.at[0], xb_b.at[0])
    exchange(1).wait_send()
    for p in range(6):
        rs_sent(p)


def hand_on(*refs):
    count = len(refs) // 2
    for source, target in zip(refs[:count], refs[count:]):
        target[...] = source[...]


def shards(features, hidden, cotangent, kernel_one, kernel_two, gains):
    T, H, W, C = features.shape
    half = kernel_one.shape[4]
    NT, NS = lax.axis_size("tm"), lax.axis_size("space")
    share = C // (NT * NS)
    R = NT * share
    WP = padded_width(W)
    wide = 9 * half

    def by_tap(kernel):
        return jnp.transpose(kernel, (1, 2, 3, 0, 4)).reshape(27, C, half)

    vmem = pl.BlockSpec(memory_space=pltpu.VMEM)
    hbm = pl.BlockSpec(memory_space=pl.ANY)
    DMA = pltpu.SemaphoreType.DMA
    call = pl.pallas_call(
        functools.partial(body, (T, H, W, C, half, NT, NS)),
        out_shape=(
            jax.ShapeDtypeStruct((T, W, H, half), BF16),
            jax.ShapeDtypeStruct((27, share, half), F32),
            jax.ShapeDtypeStruct((27, share, half), F32),
            jax.ShapeDtypeStruct((2, half), F32),
        ),
        in_specs=[hbm] * 5 + [vmem],
        out_specs=(vmem,) * 4,
        scratch_shapes=[
            pltpu.VMEM((T, W, H, C), BF16),
            pltpu.VMEM((T, W, H, C), BF16),
            pltpu.VMEM((T, W, H, C), BF16),
            pltpu.VMEM((T, H, W, C), BF16),
            pltpu.VMEM((T, H, W, C), BF16),
            pltpu.VMEM((27, C, half), BF16),
            pltpu.VMEM((27, C, half), BF16),
            pltpu.VMEM((2 * T, H + 2, W, half), BF16),
            pltpu.VMEM((2 * T, H + 2, W, half), BF16),
            pltpu.VMEM((W, H, C), F32),
            pltpu.VMEM((T, W, H, half), F32),
            pltpu.VMEM((WP + 16, half), F32),
            pltpu.VMEM((2 * T, H + 2, WP, 3 * half), BF16),
            pltpu.VMEM((T * H, WP, C), BF16),
            pltpu.VMEM((C, T * H * WP), BF16),
            pltpu.VMEM((C, C), BF16),
            pltpu.VMEM((C, C), F32),
            pltpu.VMEM((C, half), F32),
            pltpu.VMEM((2, T * H, WP, half), F32),
            pltpu.VMEM((2, T * H, WP, half), F32),
            pltpu.VMEM((T * H, WP, half), F32),
            pltpu.VMEM((8, C), F32),
            pltpu.VMEM((NT, 4, half), F32),
            pltpu.VMEM((NS, 4, half), F32),
            pltpu.VMEM((2, NT, 2, half), F32),
            pltpu.VMEM((2, NS, 2, half), F32),
            pltpu.VMEM((6, C, wide), BF16),
            pltpu.VMEM((6, 2, R // 2, wide), BF16),
            pltpu.VMEM((6, 2, R, wide), BF16),
            pltpu.VMEM((R, wide), F32),
            pltpu.VMEM((6, 2, NT // 2, share, wide), F32),
            pltpu.VMEM((6, 2, NT // 2, share, wide), BF16),
            pltpu.VMEM((6, NT // 2, share, wide), BF16),
            pltpu.VMEM((6, NT // 2, share, wide), BF16),
            pltpu.VMEM((6, NT // 2 - 1, share, wide), BF16),
            DMA((5,)),
            DMA((2, 5)),
            DMA((2, 5)),
            DMA((3, 2)),
            DMA((3, 2)),
            DMA((2,)),
            DMA((2,)),
            DMA((6, 2)),
            DMA((6, 2)),
            DMA((6, 2)),
            DMA((6, 2)),
            DMA((6,)),
            DMA((6,)),
            DMA((6,)),
            DMA((6,)),
        ],
        compiler_params=pltpu.CompilerParams(
            collective_id=0, has_side_effects=True, vmem_limit_bytes=60 * 1024 * 1024
        ),
        name="block_back",
    )
    def by_column(field):
        return jnp.transpose(field, (0, 2, 1, 3))

    made = call(
        by_column(features), by_column(hidden), by_column(cotangent),
        by_tap(kernel_one), by_tap(kernel_two), gains,
    )
    fgrad, d1, d2, gg = pl.pallas_call(
        hand_on,
        out_shape=tuple(jax.ShapeDtypeStruct(x.shape, x.dtype) for x in made),
        in_specs=[vmem] * 4,
        out_specs=(vmem,) * 4,
        name="hand_on",
    )(*made)

    def by_channel(delta):
        return jnp.transpose(delta.reshape(3, 3, 3, share, half), (3, 0, 1, 2, 4))

    return (by_column(fgrad), by_channel(d1), by_channel(d2), gg)


def solution(mesh):
    placed = (
        P(("clip", "tm"), "space", None, None),
        P(("clip", "tm"), "space", None, None),
        P(("clip", "tm"), "space", None, None),
        P(None, None, None, None, "chan"),
        P(None, None, None, None, "chan"),
        P(),
    )
    return jax.shard_map(
        shards,
        mesh=mesh,
        in_specs=placed,
        out_specs=(
            P(("clip", "tm"), "space", None, "chan"),
            P(("clip", "tm", "space"), None, None, None, "chan"),
            P(("clip", "tm", "space"), None, None, None, "chan"),
            P("clip", "chan"),
        ),
        check_vma=False,
    )
```

```python
import functools

import jax
import jax.numpy as jnp
from jax import lax
from jax.experimental import pallas as pl
from jax.experimental.pallas import tpu as pltpu
from jax.sharding import PartitionSpec as P

GROUPS = 32
PIECES = ((0, 0, 3), (1, 0, 3), (2, 0, 3), (3, 0, 3), (4, 0, 3), (5, 0, 1), (5, 1, 2), (5, 2, 3))
EPS = 1e-06
MESH = pl.DeviceIdType.MESH
F32 = jnp.float32
BF16 = jnp.bfloat16


def padded_width(width):
    return (width + 2 + 15) // 16 * 16


def body(
    dims,
    feat_hbm, hid_hbm, cot_hbm, k1_hbm, k2_hbm, gains,
    fgrad, d1, d2, gg,
    feat_n, hid_n, cot_n, feat, hid, k1, k2,
    graw2, graw1, turn, turn_half, tmp, ext, act, act_t, perm, block_sum, spread_sum,
    acc, acc_in, slope, stats,
    zb_a, xb_a, zb_b, xb_b,
    xs, xa, xb, zf, zk, zs, za, zc, zr, ring, ring_k, ring_s, ring_r,
    in_sem, halo_s, halo_r, ar_s, ar_r, ch_s, ch_r,
    xa_s, xa_r, xb_s, xb_r, za_s, za_r, z_s, z_r, hop_s, hop_r, last_s, last_r,
):
    T, H, W, C, half, NT, NS = dims
    WP = padded_width(W)
    per = C // GROUPS
    share = C // (NT * NS)
    R = NT * share
    members = float(T * H * W * per * NT * NS)
    tm, sp, ch = lax.axis_index("tm"), lax.axis_index("space"), lax.axis_index("chan")
    off = pl.multiple_of(ch * half, half)
    wide = 9 * half
    K3 = 3 * half

    def at_z(d):
        return lax.rem(tm + d, NT)

    def at_x(d):
        return lax.rem(sp + d, NS)

    def signal(barrier, where):
        pl.semaphore_signal(barrier, inc=1, device_id=where, device_id_type=MESH)

    def remote(src, dst, s, r, where):
        return pltpu.make_async_remote_copy(
            src_ref=src, dst_ref=dst, send_sem=s, recv_sem=r, device_id=where, device_id_type=MESH
        )

    loads = [
        pltpu.make_async_copy(src, dst, in_sem.at[i])
        for i, (src, dst) in enumerate(
            ((feat_hbm, feat_n), (hid_hbm, hid_n), (cot_hbm, cot_n), (k2_hbm, k2), (k1_hbm, k1))
        )
    ]
    for load in loads:
        load.start()

    barrier = pltpu.get_barrier_semaphore()

    @pl.loop(1, NT)
    def _(d):
        signal(barrier, {"tm": at_z(d)})

    for d in range(1, NS):
        signal(barrier, {"space": at_x(d)})
    signal(barrier, {"chan": 1 - ch})
    for dt in (1, NT - 1):
        for ds in (1, NS - 1):
            signal(barrier, {"tm": at_z(dt), "space": at_x(ds)})

    def group_sum(values, width):
        return lax.dot_general(
            values, block_sum[0:width, 0:width], (((1,), (0,)), ((), ())),
            precision=lax.Precision.HIGHEST, preferred_element_type=F32,
        )

    def row_of(j):
        return j // H, lax.rem(j, H)

    for load in loads[:3]:
        load.wait()

    rows = lax.broadcasted_iota(jnp.int32, (C, half), 0)
    cols = lax.broadcasted_iota(jnp.int32, (C, half), 1)
    spread_sum[...] = jnp.where(rows // per == cols, 1.0, 0.0).astype(F32)
    strip = W // 9 if W % 9 == 0 else 1

    def stat_strip(j, carry):
        t, w = j // (W // strip), lax.rem(j, W // strip) * strip
        out = []
        for k, ref in enumerate((feat_n, hid_n)):
            x = ref[t, pl.ds(w, strip)].astype(F32)
            out.append(carry[2 * k] + jnp.sum(x, axis=0))
            out.append(carry[2 * k + 1] + jnp.sum(x * x, axis=0))
        return tuple(out)

    sums = lax.fori_loop(0, T * (W // strip), stat_strip, (jnp.zeros((H, C), F32),) * 4)
    sums = jnp.concatenate([jnp.sum(x, axis=0, keepdims=True) for x in sums], axis=0)
    zb_a[tm] = lax.dot_general(
        sums, spread_sum[...], (((1,), (0,)), ((), ())),
        precision=lax.Precision.HIGHEST, preferred_element_type=F32,
    )
    for t in range(T):
        turn_half[t] = cot_n[t, :, :, pl.ds(off, half)].astype(F32)
        for h in range(H):
            graw2[t, h + 1] = turn_half[t, :, h, :].astype(BF16)
    pl.semaphore_wait(barrier, (NT - 1) + (NS - 1) + 1 + 4)

    def along_z(n, zb):
        @pl.loop(0, NT - 1)
        def _(k):
            step = (k + 1) // 2
            d = NT // 2 + jnp.where(lax.rem(k, 2) == 0, step, -step)
            remote(zb.at[tm], zb.at[tm], ar_s.at[n, 0], ar_r.at[n, 0], {"tm": at_z(d)}).start()

    def z_to_x(n, zb, xbuf):
        every = remote(
            zb.at[0 : NT - 1], zb.at[0 : NT - 1], ar_s.at[n, 0], ar_r.at[n, 0], {"tm": at_z(1)}
        )
        every.wait_recv()
        total = lax.fori_loop(1, NT, lambda j, c: c + zb[j], zb[0])
        xbuf[sp] = total
        for d in range(1, NS):
            remote(xbuf.at[sp], xbuf.at[sp], ar_s.at[n, 1], ar_r.at[n, 1], {"space": at_x(d)}).start()

    def x_total(n, zb, xbuf):
        last = remote(
            xbuf.at[0 : NS - 1], xbuf.at[0 : NS - 1], ar_s.at[n, 1], ar_r.at[n, 1], {"space": at_x(1)}
        )
        last.wait_recv()
        total = xbuf[0]
        for j in range(1, NS):
            total = total + xbuf[j]
        return total

    def reduced_sent(n, zb, xbuf):
        remote(
            zb.at[0 : NT - 1], zb.at[0 : NT - 1], ar_s.at[n, 0], ar_r.at[n, 0], {"tm": at_z(1)}
        ).wait_send()
        remote(
            xbuf.at[0 : NS - 1], xbuf.at[0 : NS - 1], ar_s.at[n, 1], ar_r.at[n, 1], {"space": at_x(1)}
        ).wait_send()

    def halo_copies(n, graw):
        right, left = at_x(1), at_x(NS - 1)
        before = at_z(NT - 1)
        own = pl.ds(0, T)
        later = pl.ds(T, T)
        plan = (
            (graw.at[own, H], graw.at[own, 0], {"space": right}),
            (graw.at[own, 1], graw.at[own, H + 1], {"space": left}),
            (graw.at[own, pl.ds(1, H)], graw.at[later, pl.ds(1, H)], {"tm": before}),
            (graw.at[own, H], graw.at[later, 0], {"tm": before, "space": right}),
            (graw.at[own, 1], graw.at[later, H + 1], {"tm": before, "space": left}),
        )
        return [
            remote(src, dst, halo_s.at[n, i], halo_r.at[n, i], where)
            for i, (src, dst, where) in enumerate(plan)
        ]

    has_right, has_left, has_before, has_after = sp < NS - 1, sp > 0, tm > 0, tm < NT - 1
    sends = (
        has_right,
        has_left,
        has_before,
        jnp.logical_and(has_before, has_right),
        jnp.logical_and(has_before, has_left),
    )
    arrives = (
        has_left,
        has_right,
        has_after,
        jnp.logical_and(has_after, has_left),
        jnp.logical_and(has_after, has_right),
    )

    def halo_start(n, graw):
        for copy, here in zip(halo_copies(n, graw), sends):
            @pl.when(here)
            def _():
                copy.start()

    def halo_wait(n, graw, which):
        copies = halo_copies(n, graw)
        for i in which:
            @pl.when(arrives[i])
            def _():
                copies[i].wait_recv()

    def halo_sent(n, graw):
        for copy, here in zip(halo_copies(n, graw), sends):
            @pl.when(here)
            def _():
                copy.wait_send()

    def place_shifted(f, r, values):
        tmp[8 : 8 + W] = values
        for c in range(3):
            ext[f, r, :, c * half : (c + 1) * half] = tmp[9 - c : 9 - c + WP].astype(BF16)

    def shift(graw, first, last):
        @pl.loop(first * (H + 2), last * (H + 2))
        def _(j):
            f, r = j // (H + 2), lax.rem(j, H + 2)
            place_shifted(f, r, graw[f, r].astype(F32))

    def taps(f, a, b):
        return ext[f + 2 - a, 2 - b : 2 - b + H].reshape(H * WP, K3)

    def back_part(kernel, f, a, first):
        left = jnp.concatenate([taps(f, a, b) for b in range(3)], axis=1)
        right = jnp.concatenate([kernel[a * 9 + k] for k in range(9)], axis=1)
        product = lax.dot_general(left, right, (((1,), (1,)), ((), ())), preferred_element_type=F32)
        for k in range(2):
            piece = product[:, k * half : (k + 1) * half].reshape(H, WP, half)
            if first:
                acc[k, f * H : (f + 1) * H] = piece
            else:
                acc[k, f * H : (f + 1) * H] += piece

    def exchange(n):
        return remote(acc.at[1 - ch], acc_in.at[n], ch_s.at[n], ch_r.at[n], {"chan": 1 - ch})

    def lanes(p):
        q, low, high = PIECES[p]
        return q, pl.ds(low * K3, (high - low) * K3)

    def delta_part(p):
        q, low, high = PIECES[p]
        a = 2 - q % 3
        for b in range(low, high):
            right = jnp.concatenate([taps(f, a, b) for f in range(T)], axis=0)
            product = lax.dot_general(
                act_t[...], right, (((1,), (0,)), ((), ())), preferred_element_type=F32
            )
            xs[q, :, b * K3 : (b + 1) * K3] = product.astype(BF16)

    def chunk(s, part, parts):
        size = R // parts
        return pl.ds(pl.multiple_of(s * R + part * size, size), size)

    def sum_1(p):
        far = at_x(2)
        q, cut = lanes(p)
        return [
            remote(
                xs.at[q, chunk(far, k, 2), cut], xa.at[q, k, :, cut],
                xa_s.at[p, k], xa_r.at[p, k], {"space": at_x(d)},
            )
            for k, d in enumerate((1, NS - 1))
        ]

    def sum_2(p):
        q, cut = lanes(p)
        return [
            remote(
                xs.at[q, chunk(at_x(d), 0, 1), cut], xb.at[q, k, :, cut],
                xb_s.at[p, k], xb_r.at[p, k], {"space": at_x(d)},
            )
            for k, d in enumerate((1, NS - 1))
        ]

    def rs_start(p):
        for copy in sum_1(p):
            copy.start()

    def rs_pass(p):
        q, cut = lanes(p)
        for k, (first, second) in enumerate(zip(sum_1(p), sum_2(p))):
            first.wait_recv()
            rows = chunk(at_x((1, NS - 1)[k]), k, 2)
            xs[q, rows, cut] = (xs[q, rows, cut].astype(F32) + xa[q, k, :, cut].astype(F32)).astype(BF16)
            second.start()

    pairs = NT // 2
    parity = lax.rem(tm, 2)
    place = tm // 2

    def mate(p):
        turned = parity if p % 2 == 0 else 1 - parity
        return {"tm": lax.rem(tm + 1 - 2 * turned + NT, NT)}

    def to_mate(p):
        q, cut = lanes(p)
        return remote(
            zs.at[q, 1 - parity, :, :, cut], za.at[q, :, :, cut], za_s.at[p], za_r.at[p], mate(p)
        )

    def rs_z1(p):
        q, cut = lanes(p)
        for copy in sum_2(p):
            copy.wait_recv()
        kept = xs[q, chunk(sp, 0, 1), cut].astype(F32)
        zf[:, cut] = kept + xb[q, 0, :, cut].astype(F32) + xb[q, 1, :, cut].astype(F32)
        for t in range(NT):
            rows = zf[t * share : (t + 1) * share, cut]
            zk[q, t % 2, t // 2, :, cut] = rows
            zs[q, t % 2, t // 2, :, cut] = rows.astype(BF16)
        to_mate(p).start()

    def rs_z2(p):
        q, cut = lanes(p)
        to_mate(p).wait_recv()

        @pl.loop(0, pairs)
        def _(j):
            both = zk[q, parity, j, :, cut] + za[q, j, :, cut].astype(F32)
            zk[q, parity, j, :, cut] = both
            zc[q, j, :, cut] = both.astype(BF16)

        @pl.loop(1, pairs)
        def _(k):
            d = lax.rem(k + pairs // 2 - 1, pairs - 1) + 1
            to = lax.rem(place + d, pairs)
            remote(
                zc.at[q, to, :, cut], zr.at[q, d - 1, :, cut], z_s.at[p], z_r.at[p],
                {"tm": 2 * to + parity},
            ).start()

    def z_all(p):
        q, cut = lanes(p)
        return remote(
            zc.at[q, pl.ds(0, pairs - 1), :, cut], zr.at[q, :, :, cut], z_s.at[p], z_r.at[p], mate(p)
        )

    def rs_end(p):
        q, low, high = PIECES[p]
        cut = lanes(p)[1]
        z_all(p).wait_recv()
        total = zk[q, parity, place, :, cut]
        for j in range(pairs - 1):
            total = total + zr[q, j, :, cut].astype(F32)
        out, a = (d2, d1)[q // 3], 2 - q % 3
        for k in range(3 * (high - low)):
            out[a * 9 + 3 * low + k] = total[:, k * half : (k + 1) * half]

    def rs_sent(p):
        for copy in sum_1(p) + sum_2(p):
            copy.wait_send()
        to_mate(p).wait_send()
        z_all(p).wait_send()

    deep = NT // 2
    band = NS * share

    def band_of(t):
        return pl.ds(pl.multiple_of(t * band, band), band)

    def hop(q, way, k):
        if way == 0:
            dest, to, slot = at_z(deep - k), at_z(1), k
        else:
            dest, to, slot = at_z(NT - deep + 1 + k), at_z(NT - 1), deep + k
        return dest, remote(
            xs.at[q, band_of(dest)], ring.at[q, slot], hop_s.at[q, slot], hop_r.at[q, slot], {"tm": to}
        )

    def tick(q, k):
        for way in range(2):
            if k >= deep - way:
                continue
            dest, copy = hop(q, way, k)
            if k > 0:
                hop(q, way, k - 1)[1].wait_recv()
                came = ring[q, way * deep + k - 1].astype(F32)
                xs[q, band_of(dest)] = (xs[q, band_of(dest)].astype(F32) + came).astype(BF16)
            copy.start()

    def ticks(k):
        for q in range(3):
            tick(q, k)

    def across(q, d):
        return remote(
            ring_s.at[q, at_x(d)], ring_r.at[q, d - 1], last_s.at[q, d - 1], last_r.at[q, d - 1],
            {"space": at_x(d)},
        )

    def ring_pass(q):
        for way in range(2):
            hop(q, way, deep - 1 - way)[1].wait_recv()
        total = xs[q, band_of(tm)].astype(F32)
        total = total + ring[q, deep - 1].astype(F32) + ring[q, 2 * deep - 2].astype(F32)
        zf[0:band] = total
        for x in range(NS):
            rows = zf[x * share : (x + 1) * share]
            ring_k[q, x] = rows
            ring_s[q, x] = rows.astype(BF16)
        for d in range(1, NS):
            across(q, d).start()

    def ring_end(q):
        total = ring_k[q, sp]
        for d in range(1, NS):
            across(q, d).wait_recv()
            total = total + ring_r[q, d - 1].astype(F32)
        for k in range(9):
            d2[(2 - q) * 9 + k] = total[:, k * half : (k + 1) * half]

    def ring_sent(q):
        for way in range(2):
            for k in range(deep - way):
                hop(q, way, k)[1].wait_send()
        for d in range(1, NS):
            across(q, d).wait_send()

    def activate(ref, n, order):
        @pl.loop(0, T * H)
        def _(j):
            t, h = row_of(j)
            scaled = (ref[t, h].astype(F32) - stats[2 * n : 2 * n + 1]) * stats[2 * n + 1 : 2 * n + 2]
            scaled = scaled * gains[n : n + 1]
            act[j, 0:W] = (scaled * jax.nn.sigmoid(scaled)).astype(BF16)

        act_t[...] = lax.dot_general(
            order, act[...].reshape(T * H * WP, C), (((1,), (1,)), ((), ())),
            preferred_element_type=F32,
        ).astype(BF16)

    def own_row(ref, k):
        return ref[k : k + 1, pl.ds(off, half)]

    def centred_row(ref, n, t, h):
        x = ref[t, h, :, pl.ds(off, half)].astype(F32)
        return (x - own_row(stats, 2 * n)) * own_row(stats, 2 * n + 1)

    def slopes(ref, n):
        exchanged = 1 - n

        def row(j, carry):
            t, h = row_of(j)
            centred = centred_row(ref, n, t, h)
            scaled = centred * own_row(gains, n)
            gate = jax.nn.sigmoid(scaled)
            upstream = acc[ch, j, 0:W] + acc_in[exchanged, j, 0:W]
            value = upstream * gate * (1.0 + scaled * (1.0 - gate))
            slope[j, 0:W] = value
            return (
                carry[0] + jnp.sum(value, axis=0, keepdims=True),
                carry[1] + jnp.sum(value * centred, axis=0, keepdims=True),
            )

        zero = jnp.zeros((1, half), F32)
        return lax.fori_loop(0, T * H, row, (zero, zero))

    def norm_terms(n, totals):
        both = group_sum(totals * own_row(gains, n), half) * (1.0 / members)
        gg[n : n + 1] = totals[1:2]
        return both[0:1], both[1:2]

    def grad_row(ref, n, t, h, terms):
        first, second = terms
        centred = centred_row(ref, n, t, h)
        inner = slope[t * H + h, 0:W] * own_row(gains, n) - first - centred * second
        return own_row(stats, 2 * n + 1) * inner

    def hidden_rows(totals):
        terms = norm_terms(1, totals)

        @pl.loop(0, T * H)
        def _(j):
            t, h = row_of(j)
            graw1[t, h + 1] = grad_row(hid, 1, t, h, terms).astype(BF16)

    def feature_rows(totals):
        terms = norm_terms(0, totals)

        @pl.loop(0, T)
        def _(t):
            for h in range(H):
                base = graw2[t, h + 1].astype(F32)
                turn_half[t, :, h, :] = base + grad_row(feat, 0, t, h, terms)
            fgrad[t] = turn_half[t].astype(BF16)

    def by_rows(source, target):
        @pl.loop(0, T)
        def _(t):
            turn[...] = source[t].astype(F32)
            for h in range(H):
                target[t, h] = turn[:, h, :].astype(BF16)

    def reduce_slopes(n, parts):
        for k in range(2):
            zb_b[n, tm, k : k + 1] = parts[k]
        along_z(2 - n, zb_b.at[n])

    along_z(0, zb_a)
    halo_start(0, graw2)
    tmp[...] = jnp.zeros_like(tmp)
    act[...] = jnp.zeros_like(act)
    for graw in (graw2, graw1):
        @pl.when(sp == 0)
        def _():
            graw[:, 0] = jnp.zeros((2 * T, W, half), BF16)

        @pl.when(sp == NS - 1)
        def _():
            graw[:, H + 1] = jnp.zeros((2 * T, W, half), BF16)

        @pl.when(tm == NT - 1)
        def _():
            graw[T : 2 * T] = jnp.zeros((T, H + 2, W, half), BF16)

    rows = lax.broadcasted_iota(jnp.int32, (C, C), 0)
    cols = lax.broadcasted_iota(jnp.int32, (C, C), 1)
    within = lax.rem(rows, R)
    source = within // share * (NS * share) + rows // R * share + lax.rem(within, share)
    perm[...] = jnp.where(cols == source, 1.0, 0.0).astype(BF16)
    same = rows == cols
    block_sum[...] = jnp.where(rows // per == cols // per, 1.0, 0.0).astype(F32)
    by_rows(hid_n, hid)
    by_rows(feat_n, feat)

    def back_parts(kernel, later):
        for f in range(T):
            for a in (2, 1, 0):
                if (f + 2 - a >= T) == later:
                    back_part(kernel, f, a, a == 2)

    halo_wait(0, graw2, (0, 1))
    shift(graw2, 0, T)
    loads[3].wait()
    back_parts(k2, False)
    z_to_x(0, zb_a, xb_a)
    halo_wait(0, graw2, (2, 3, 4))
    shift(graw2, T, 2 * T)
    back_parts(k2, True)
    exchange(0).start()
    totals = lax.dot_general(
        x_total(0, zb_a, xb_a), spread_sum[...], (((1,), (1,)), ((), ())),
        precision=lax.Precision.HIGHEST, preferred_element_type=F32,
    ) * (1.0 / members)
    for n in range(2):
        mean = totals[2 * n : 2 * n + 1]
        spread = totals[2 * n + 1 : 2 * n + 2] - mean * mean
        stats[2 * n : 2 * n + 1] = mean
        stats[2 * n + 1 : 2 * n + 2] = lax.rsqrt(spread + EPS)
    exchange(0).wait_recv()
    reduce_slopes(1, slopes(hid, 1))
    activate(hid, 1, jnp.where(same, 1.0, 0.0).astype(BF16))
    for p in range(3):
        delta_part(p)
        tick(p, 0)
    activate(feat, 0, perm[...])
    z_to_x(1, zb_b.at[1], xb_b.at[1])
    ticks(1)
    totals_two = x_total(1, zb_b.at[1], xb_b.at[1])

    hidden_rows(totals_two)
    halo_start(1, graw1)
    ticks(2)
    halo_wait(1, graw1, (0, 1))
    shift(graw1, 0, T)
    delta_part(3)
    rs_start(3)
    loads[4].wait()
    exchange(0).wait_send()
    back_parts(k1, False)
    ticks(3)
    halo_wait(1, graw1, (2, 3, 4))
    shift(graw1, T, 2 * T)
    for p in range(4, 8):
        delta_part(p)
        rs_start(p)
    rs_pass(3)
    ticks(4)
    back_parts(k1, True)
    exchange(1).start()
    rs_pass(4)
    for p in range(5, 8):
        rs_pass(p)
    ticks(5)
    exchange(1).wait_recv()
    reduce_slopes(0, slopes(feat, 0))
    rs_z1(3)
    ticks(6)
    rs_z1(4)
    for p in range(5, 8):
        rs_z1(p)
    ticks(7)
    rs_z2(3)
    rs_z2(4)
    z_to_x(2, zb_b.at[0], xb_b.at[0])
    for p in range(5, 8):
        rs_z2(p)
    for q in range(3):
        ring_pass(q)
    feature_rows(x_total(2, zb_b.at[0], xb_b.at[0]))
    for q in range(3):
        ring_end(q)
    for p in range(3, 8):
        rs_end(p)

    halo_sent(0, graw2)
    halo_sent(1, graw1)
    reduced_sent(0, zb_a, xb_a)
    reduced_sent(1, zb_b.at[1], xb_b.at[1])
    reduced_sent(2, zb_b.at[0], xb_b.at[0])
    exchange(1).wait_send()
    for p in range(3, 8):
        rs_sent(p)
    for q in range(3):
        ring_sent(q)


def hand_on(*refs):
    count = len(refs) // 2
    for source, target in zip(refs[:count], refs[count:]):
        target[...] = source[...]


def shards(features, hidden, cotangent, kernel_one, kernel_two, gains):
    T, H, W, C = features.shape
    half = kernel_one.shape[4]
    NT, NS = lax.axis_size("tm"), lax.axis_size("space")
    share = C // (NT * NS)
    R = NT * share
    WP = padded_width(W)
    wide = 9 * half

    def by_tap(kernel):
        return jnp.transpose(kernel, (1, 2, 3, 0, 4)).reshape(27, C, half)

    vmem = pl.BlockSpec(memory_space=pltpu.VMEM)
    hbm = pl.BlockSpec(memory_space=pl.ANY)
    DMA = pltpu.SemaphoreType.DMA
    call = pl.pallas_call(
        functools.partial(body, (T, H, W, C, half, NT, NS)),
        out_shape=(
            jax.ShapeDtypeStruct((T, W, H, half), BF16),
            jax.ShapeDtypeStruct((27, share, half), F32),
            jax.ShapeDtypeStruct((27, share, half), F32),
            jax.ShapeDtypeStruct((2, half), F32),
        ),
        in_specs=[hbm] * 5 + [vmem],
        out_specs=(vmem,) * 4,
        scratch_shapes=[
            pltpu.VMEM((T, W, H, C), BF16),
            pltpu.VMEM((T, W, H, C), BF16),
            pltpu.VMEM((T, W, H, C), BF16),
            pltpu.VMEM((T, H, W, C), BF16),
            pltpu.VMEM((T, H, W, C), BF16),
            pltpu.VMEM((27, C, half), BF16),
            pltpu.VMEM((27, C, half), BF16),
            pltpu.VMEM((2 * T, H + 2, W, half), BF16),
            pltpu.VMEM((2 * T, H + 2, W, half), BF16),
            pltpu.VMEM((W, H, C), F32),
            pltpu.VMEM((T, W, H, half), F32),
            pltpu.VMEM((WP + 16, half), F32),
            pltpu.VMEM((2 * T, H + 2, WP, 3 * half), BF16),
            pltpu.VMEM((T * H, WP, C), BF16),
            pltpu.VMEM((C, T * H * WP), BF16),
            pltpu.VMEM((C, C), BF16),
            pltpu.VMEM((C, C), F32),
            pltpu.VMEM((C, half), F32),
            pltpu.VMEM((2, T * H, WP, half), F32),
            pltpu.VMEM((2, T * H, WP, half), F32),
            pltpu.VMEM((T * H, WP, half), F32),
            pltpu.VMEM((8, C), F32),
            pltpu.VMEM((NT, 4, half), F32),
            pltpu.VMEM((NS, 4, half), F32),
            pltpu.VMEM((2, NT, 2, half), F32),
            pltpu.VMEM((2, NS, 2, half), F32),
            pltpu.VMEM((6, C, wide), BF16),
            pltpu.VMEM((6, 2, R // 2, wide), BF16),
            pltpu.VMEM((6, 2, R, wide), BF16),
            pltpu.VMEM((R, wide), F32),
            pltpu.VMEM((6, 2, NT // 2, share, wide), F32),
            pltpu.VMEM((6, 2, NT // 2, share, wide), BF16),
            pltpu.VMEM((6, NT // 2, share, wide), BF16),
            pltpu.VMEM((6, NT // 2, share, wide), BF16),
            pltpu.VMEM((6, NT // 2 - 1, share, wide), BF16),
            pltpu.VMEM((3, NT - 1, NS * share, wide), BF16),
            pltpu.VMEM((3, NS, share, wide), F32),
            pltpu.VMEM((3, NS, share, wide), BF16),
            pltpu.VMEM((3, NS - 1, share, wide), BF16),
            DMA((5,)),
            DMA((2, 5)),
            DMA((2, 5)),
            DMA((3, 2)),
            DMA((3, 2)),
            DMA((2,)),
            DMA((2,)),
            DMA((8, 2)),
            DMA((8, 2)),
            DMA((8, 2)),
            DMA((8, 2)),
            DMA((8,)),
            DMA((8,)),
            DMA((8,)),
            DMA((8,)),
            DMA((3, NT - 1)),
            DMA((3, NT - 1)),
            DMA((3, NS - 1)),
            DMA((3, NS - 1)),
        ],
        compiler_params=pltpu.CompilerParams(
            collective_id=0, has_side_effects=True, vmem_limit_bytes=60 * 1024 * 1024
        ),
        name="block_back",
    )
    def by_column(field):
        return jnp.transpose(field, (0, 2, 1, 3))

    made = call(
        by_column(features), by_column(hidden), by_column(cotangent),
        by_tap(kernel_one), by_tap(kernel_two), gains,
    )
    fgrad, d1, d2, gg = pl.pallas_call(
        hand_on,
        out_shape=tuple(jax.ShapeDtypeStruct(x.shape, x.dtype) for x in made),
        in_specs=[vmem] * 4,
        out_specs=(vmem,) * 4,
        name="hand_on",
    )(*made)

    def by_channel(delta):
        return jnp.transpose(delta.reshape(3, 3, 3, share, half), (3, 0, 1, 2, 4))

    return (by_column(fgrad), by_channel(d1), by_channel(d2), gg)


def solution(mesh):
    placed = (
        P(("clip", "tm"), "space", None, None),
        P(("clip", "tm"), "space", None, None),
        P(("clip", "tm"), "space", None, None),
        P(None, None, None, None, "chan"),
        P(None, None, None, None, "chan"),
        P(),
    )
    return jax.shard_map(
        shards,
        mesh=mesh,
        in_specs=placed,
        out_specs=(
            P(("clip", "tm"), "space", None, "chan"),
            P(("clip", "tm", "space"), None, None, None, "chan"),
            P(("clip", "tm", "space"), None, None, None, "chan"),
            P("clip", "chan"),
        ),
        check_vma=False,
    )
```

```python
import functools

import jax
import jax.numpy as jnp
from jax import lax
from jax.experimental import pallas as pl
from jax.experimental.pallas import tpu as pltpu
from jax.sharding import PartitionSpec as P

GROUPS = 32
PIECES = ((0, 0, 3), (1, 0, 3), (2, 0, 3), (3, 0, 3), (4, 0, 3), (5, 0, 1), (5, 1, 2), (5, 2, 3))
EPS = 1e-06
MESH = pl.DeviceIdType.MESH
F32 = jnp.float32
BF16 = jnp.bfloat16


def padded_width(width):
    return (width + 2 + 15) // 16 * 16


def body(
    dims,
    feat_hbm, hid_hbm, cot_hbm, k1_hbm, k2_hbm, gains,
    fgrad, d1, d2, gg,
    feat_n, hid_n, cot_n, wide_feat, hid, k1, k2,
    graw2, graw1, turn, turn_half, tmp, ext, act, act_t, wide_act, wide_act_t, own_f, perm, block_sum, spread_sum,
    acc, acc_in, slope, stats,
    zb_a, xb_a, zb_b, xb_b,
    xs, xa, xb, zf, zk, zs, za, zc, zr, ring, ring_k, ring_s, ring_r,
    in_sem, halo_s, halo_r, ar_s, ar_r, ch_s, ch_r,
    xa_s, xa_r, xb_s, xb_r, za_s, za_r, z_s, z_r, hop_s, hop_r, last_s, last_r,
):
    T, H, W, C, half, NT, NS = dims
    WP = padded_width(W)
    per = C // GROUPS
    share = C // (NT * NS)
    R = NT * share
    members = float(T * H * W * per * NT * NS)
    tm, sp, ch = lax.axis_index("tm"), lax.axis_index("space"), lax.axis_index("chan")
    off = pl.multiple_of(ch * half, half)
    wide = 9 * half
    K3 = 3 * half
    feat = wide_feat.at[pl.ds(T, T), pl.ds(1, H)]

    def at_z(d):
        return lax.rem(tm + d, NT)

    def at_x(d):
        return lax.rem(sp + d, NS)

    def signal(barrier, where):
        pl.semaphore_signal(barrier, inc=1, device_id=where, device_id_type=MESH)

    def remote(src, dst, s, r, where):
        return pltpu.make_async_remote_copy(
            src_ref=src, dst_ref=dst, send_sem=s, recv_sem=r, device_id=where, device_id_type=MESH
        )

    loads = [
        pltpu.make_async_copy(src, dst, in_sem.at[i])
        for i, (src, dst) in enumerate(
            ((feat_hbm, feat_n), (hid_hbm, hid_n), (cot_hbm, cot_n), (k2_hbm, k2), (k1_hbm, k1))
        )
    ]
    for load in loads:
        load.start()

    barrier = pltpu.get_barrier_semaphore()

    @pl.loop(1, NT)
    def _(d):
        signal(barrier, {"tm": at_z(d)})

    for d in range(1, NS):
        signal(barrier, {"space": at_x(d)})
    signal(barrier, {"chan": 1 - ch})
    for dt in (1, NT - 1):
        for ds in (1, NS - 1):
            signal(barrier, {"tm": at_z(dt), "space": at_x(ds)})

    def group_sum(values, width):
        return lax.dot_general(
            values, block_sum[0:width, 0:width], (((1,), (0,)), ((), ())),
            precision=lax.Precision.HIGHEST, preferred_element_type=F32,
        )

    def row_of(j):
        return j // H, lax.rem(j, H)

    for load in loads[:3]:
        load.wait()

    rows = lax.broadcasted_iota(jnp.int32, (C, half), 0)
    cols = lax.broadcasted_iota(jnp.int32, (C, half), 1)
    spread_sum[...] = jnp.where(rows // per == cols, 1.0, 0.0).astype(F32)
    strip = W // 9 if W % 9 == 0 else 1

    def stat_strip(j, carry):
        t, w = j // (W // strip), lax.rem(j, W // strip) * strip
        out = []
        for k, ref in enumerate((feat_n, hid_n)):
            x = ref[t, pl.ds(w, strip)].astype(F32)
            out.append(carry[2 * k] + jnp.sum(x, axis=0))
            out.append(carry[2 * k + 1] + jnp.sum(x * x, axis=0))
        return tuple(out)

    sums = lax.fori_loop(0, T * (W // strip), stat_strip, (jnp.zeros((H, C), F32),) * 4)
    sums = jnp.concatenate([jnp.sum(x, axis=0, keepdims=True) for x in sums], axis=0)
    zb_a[tm] = lax.dot_general(
        sums, spread_sum[...], (((1,), (0,)), ((), ())),
        precision=lax.Precision.HIGHEST, preferred_element_type=F32,
    )
    for t in range(T):
        turn_half[t] = cot_n[t, :, :, pl.ds(off, half)].astype(F32)
        for h in range(H):
            graw2[t, h + 1] = turn_half[t, :, h, :].astype(BF16)
    pl.semaphore_wait(barrier, (NT - 1) + (NS - 1) + 1 + 4)

    def along_z(n, zb):
        @pl.loop(0, NT - 1)
        def _(k):
            step = (k + 1) // 2
            d = NT // 2 + jnp.where(lax.rem(k, 2) == 0, step, -step)
            remote(zb.at[tm], zb.at[tm], ar_s.at[n, 0], ar_r.at[n, 0], {"tm": at_z(d)}).start()

    def z_to_x(n, zb, xbuf):
        every = remote(
            zb.at[0 : NT - 1], zb.at[0 : NT - 1], ar_s.at[n, 0], ar_r.at[n, 0], {"tm": at_z(1)}
        )
        every.wait_recv()
        total = lax.fori_loop(1, NT, lambda j, c: c + zb[j], zb[0])
        xbuf[sp] = total
        for d in range(1, NS):
            remote(xbuf.at[sp], xbuf.at[sp], ar_s.at[n, 1], ar_r.at[n, 1], {"space": at_x(d)}).start()

    def x_total(n, zb, xbuf):
        last = remote(
            xbuf.at[0 : NS - 1], xbuf.at[0 : NS - 1], ar_s.at[n, 1], ar_r.at[n, 1], {"space": at_x(1)}
        )
        last.wait_recv()
        total = xbuf[0]
        for j in range(1, NS):
            total = total + xbuf[j]
        return total

    def reduced_sent(n, zb, xbuf):
        remote(
            zb.at[0 : NT - 1], zb.at[0 : NT - 1], ar_s.at[n, 0], ar_r.at[n, 0], {"tm": at_z(1)}
        ).wait_send()
        remote(
            xbuf.at[0 : NS - 1], xbuf.at[0 : NS - 1], ar_s.at[n, 1], ar_r.at[n, 1], {"space": at_x(1)}
        ).wait_send()

    def halo_copies(n, graw):
        right, left = at_x(1), at_x(NS - 1)
        before = at_z(NT - 1)
        own = pl.ds(0, T)
        later = pl.ds(T, T)
        plan = (
            (graw.at[own, H], graw.at[own, 0], {"space": right}),
            (graw.at[own, 1], graw.at[own, H + 1], {"space": left}),
            (graw.at[own, pl.ds(1, H)], graw.at[later, pl.ds(1, H)], {"tm": before}),
            (graw.at[own, H], graw.at[later, 0], {"tm": before, "space": right}),
            (graw.at[own, 1], graw.at[later, H + 1], {"tm": before, "space": left}),
        )
        return [
            remote(src, dst, halo_s.at[n, i], halo_r.at[n, i], where)
            for i, (src, dst, where) in enumerate(plan)
        ]

    has_right, has_left, has_before, has_after = sp < NS - 1, sp > 0, tm > 0, tm < NT - 1
    sends = (
        has_right,
        has_left,
        has_before,
        jnp.logical_and(has_before, has_right),
        jnp.logical_and(has_before, has_left),
    )
    arrives = (
        has_left,
        has_right,
        has_after,
        jnp.logical_and(has_after, has_left),
        jnp.logical_and(has_after, has_right),
    )

    def halo_start(n, graw):
        for copy, here in zip(halo_copies(n, graw), sends):
            @pl.when(here)
            def _():
                copy.start()

    def halo_wait(n, graw, which):
        copies = halo_copies(n, graw)
        for i in which:
            @pl.when(arrives[i])
            def _():
                copies[i].wait_recv()

    def halo_sent(n, graw):
        for copy, here in zip(halo_copies(n, graw), sends):
            @pl.when(here)
            def _():
                copy.wait_send()

    def feature_copies():
        right, left, after = at_x(1), at_x(NS - 1), at_z(1)
        own, earlier = pl.ds(T, T), pl.ds(0, T)
        w = wide_feat
        plan = (
            (w.at[own, H], w.at[own, 0], {"space": right}),
            (w.at[own, 1], w.at[own, H + 1], {"space": left}),
            (w.at[own, pl.ds(1, H)], w.at[earlier, pl.ds(1, H)], {"tm": after}),
            (w.at[own, H], w.at[earlier, 0], {"tm": after, "space": right}),
            (w.at[own, 1], w.at[earlier, H + 1], {"tm": after, "space": left}),
        )
        return [
            remote(src, dst, halo_s.at[2, i], halo_r.at[2, i], where)
            for i, (src, dst, where) in enumerate(plan)
        ]

    feature_sends = (
        has_right,
        has_left,
        has_after,
        jnp.logical_and(has_after, has_right),
        jnp.logical_and(has_after, has_left),
    )
    feature_arrives = (
        has_left,
        has_right,
        has_before,
        jnp.logical_and(has_before, has_left),
        jnp.logical_and(has_before, has_right),
    )

    def feature_start():
        for copy, here in zip(feature_copies(), feature_sends):
            @pl.when(here)
            def _():
                copy.start()

    def feature_wait():
        for copy, here in zip(feature_copies(), feature_arrives):
            @pl.when(here)
            def _():
                copy.wait_recv()

    def feature_sent():
        for copy, here in zip(feature_copies(), feature_sends):
            @pl.when(here)
            def _():
                copy.wait_send()

    def place_shifted(f, r, values):
        tmp[8 : 8 + W] = values
        for c in range(3):
            ext[f, r, :, c * half : (c + 1) * half] = tmp[9 - c : 9 - c + WP].astype(BF16)

    def shift(graw, first, last):
        @pl.loop(first * (H + 2), last * (H + 2))
        def _(j):
            f, r = j // (H + 2), lax.rem(j, H + 2)
            place_shifted(f, r, graw[f, r].astype(F32))

    def shift_own(graw):
        @pl.loop(0, T * H)
        def _(j):
            place_shifted(j // H, lax.rem(j, H) + 1, graw[j // H, lax.rem(j, H) + 1].astype(F32))

    def shift_edges(graw):
        @pl.loop(0, 2 * T)
        def _(j):
            f, r = j // 2, lax.rem(j, 2) * (H + 1)
            place_shifted(f, r, graw[f, r].astype(F32))

    def taps(f, a, b):
        return ext[f + 2 - a, 2 - b : 2 - b + H].reshape(H * WP, K3)

    def back_part(kernel, f, a, first):
        left = jnp.concatenate([taps(f, a, b) for b in range(3)], axis=1)
        right = jnp.concatenate([kernel[a * 9 + k] for k in range(9)], axis=1)
        product = lax.dot_general(left, right, (((1,), (1,)), ((), ())), preferred_element_type=F32)
        for k in range(2):
            piece = product[:, k * half : (k + 1) * half].reshape(H, WP, half)
            if first:
                acc[k, f * H : (f + 1) * H] = piece
            else:
                acc[k, f * H : (f + 1) * H] += piece

    def exchange(n):
        return remote(acc.at[1 - ch], acc_in.at[n], ch_s.at[n], ch_r.at[n], {"chan": 1 - ch})

    def lanes(p):
        q, low, high = PIECES[p]
        return q, pl.ds(low * K3, (high - low) * K3)

    def delta_part(p):
        q, low, high = PIECES[p]
        a = 2 - q % 3
        for b in range(low, high):
            if q < 3:
                left = act_t[...]
                right = jnp.concatenate([taps(f, a, b) for f in range(T)], axis=0)
            else:
                left = wide_act_t[b, :, a * H * WP : (a + T) * H * WP]
                right = jnp.concatenate([taps(f, 2, 1) for f in range(T)], axis=0)
            product = lax.dot_general(
                left, right, (((1,), (0,)), ((), ())), preferred_element_type=F32
            )
            xs[q, :, b * K3 : (b + 1) * K3] = product.astype(BF16)
            if q < 3:
                own_f[q, :, b * K3 : (b + 1) * K3] = product

    def chunk(s, part, parts):
        size = R // parts
        return pl.ds(pl.multiple_of(s * R + part * size, size), size)

    def sum_1(p):
        far = at_x(2)
        q, cut = lanes(p)
        return [
            remote(
                xs.at[q, chunk(far, k, 2), cut], xa.at[q, k, :, cut],
                xa_s.at[p, k], xa_r.at[p, k], {"space": at_x(d)},
            )
            for k, d in enumerate((1, NS - 1))
        ]

    def sum_2(p):
        q, cut = lanes(p)
        return [
            remote(
                xs.at[q, chunk(at_x(d), 0, 1), cut], xb.at[q, k, :, cut],
                xb_s.at[p, k], xb_r.at[p, k], {"space": at_x(d)},
            )
            for k, d in enumerate((1, NS - 1))
        ]

    def rs_start(p):
        for copy in sum_1(p):
            copy.start()

    def rs_pass(p):
        q, cut = lanes(p)
        for k, (first, second) in enumerate(zip(sum_1(p), sum_2(p))):
            first.wait_recv()
            rows = chunk(at_x((1, NS - 1)[k]), k, 2)
            xs[q, rows, cut] = (xs[q, rows, cut].astype(F32) + xa[q, k, :, cut].astype(F32)).astype(BF16)
            second.start()

    pairs = NT // 2
    parity = lax.rem(tm, 2)
    place = tm // 2

    def mate(p):
        turned = parity if p % 2 == 0 else 1 - parity
        return {"tm": lax.rem(tm + 1 - 2 * turned + NT, NT)}

    def to_mate(p):
        q, cut = lanes(p)
        return remote(
            zs.at[q, 1 - parity, :, :, cut], za.at[q, :, :, cut], za_s.at[p], za_r.at[p], mate(p)
        )

    def rs_z1(p):
        q, cut = lanes(p)
        for copy in sum_2(p):
            copy.wait_recv()
        kept = xs[q, chunk(sp, 0, 1), cut].astype(F32)
        zf[:, cut] = kept + xb[q, 0, :, cut].astype(F32) + xb[q, 1, :, cut].astype(F32)
        for t in range(NT):
            rows = zf[t * share : (t + 1) * share, cut]
            zk[q, t % 2, t // 2, :, cut] = rows
            zs[q, t % 2, t // 2, :, cut] = rows.astype(BF16)
        to_mate(p).start()

    def rs_z2(p):
        q, cut = lanes(p)
        to_mate(p).wait_recv()

        @pl.loop(0, pairs)
        def _(j):
            both = zk[q, parity, j, :, cut] + za[q, j, :, cut].astype(F32)
            zk[q, parity, j, :, cut] = both
            zc[q, j, :, cut] = both.astype(BF16)

        @pl.loop(1, pairs)
        def _(k):
            d = lax.rem(k + pairs // 2 - 1, pairs - 1) + 1
            to = lax.rem(place + d, pairs)
            remote(
                zc.at[q, to, :, cut], zr.at[q, d - 1, :, cut], z_s.at[p], z_r.at[p],
                {"tm": 2 * to + parity},
            ).start()

    def z_all(p):
        q, cut = lanes(p)
        return remote(
            zc.at[q, pl.ds(0, pairs - 1), :, cut], zr.at[q, :, :, cut], z_s.at[p], z_r.at[p], mate(p)
        )

    def rs_end(p):
        q, low, high = PIECES[p]
        cut = lanes(p)[1]
        z_all(p).wait_recv()
        total = zk[q, parity, place, :, cut]
        for j in range(pairs - 1):
            total = total + zr[q, j, :, cut].astype(F32)
        out, a = (d2, d1)[q // 3], 2 - q % 3
        for k in range(3 * (high - low)):
            out[a * 9 + 3 * low + k] = total[:, k * half : (k + 1) * half]

    def rs_sent(p):
        for copy in sum_1(p) + sum_2(p):
            copy.wait_send()
        to_mate(p).wait_send()
        z_all(p).wait_send()

    steps = (NT // 2, NT - 1 - NT // 2)
    band = NS * share

    def band_of(t):
        return pl.ds(pl.multiple_of(t * band, band), band)

    def hop(q, way, k):
        if way == 0:
            dest, to, slot = at_z(steps[0] - k), at_z(1), k
        else:
            dest, to, slot = at_z(NT - steps[1] + k), at_z(NT - 1), steps[0] + k
        return dest, remote(
            xs.at[q, band_of(dest)], ring.at[q, slot], hop_s.at[q, slot], hop_r.at[q, slot], {"tm": to}
        )

    def tick(q, way, k):
        dest, copy = hop(q, way, k)
        if k > 0:
            hop(q, way, k - 1)[1].wait_recv()
            came = ring[q, way * steps[0] + k - 1].astype(F32)
            xs[q, band_of(dest)] = (own_f[q, band_of(dest)] + came).astype(BF16)
        copy.start()

    def ticks(way, k):
        for q in range(3):
            tick(q, way, k)

    def across(q, d):
        return remote(
            ring_s.at[q, at_x(d)], ring_r.at[q, d - 1], last_s.at[q, d - 1], last_r.at[q, d - 1],
            {"space": at_x(d)},
        )

    def ring_pass(q):
        for way in range(2):
            hop(q, way, steps[way] - 1)[1].wait_recv()
        total = own_f[q, band_of(tm)]
        total = total + ring[q, steps[0] - 1].astype(F32) + ring[q, NT - 2].astype(F32)
        zf[0:band] = total
        for x in range(NS):
            rows = zf[x * share : (x + 1) * share]
            ring_k[q, x] = rows
            ring_s[q, x] = rows.astype(BF16)
        for d in range(1, NS):
            across(q, d).start()

    def ring_end(q):
        total = ring_k[q, sp]
        for d in range(1, NS):
            across(q, d).wait_recv()
            total = total + ring_r[q, d - 1].astype(F32)
        for k in range(9):
            d2[(2 - q) * 9 + k] = total[:, k * half : (k + 1) * half]

    def ring_sent(q):
        for way in range(2):
            for k in range(steps[way]):
                hop(q, way, k)[1].wait_send()
        for d in range(1, NS):
            across(q, d).wait_send()

    def activated(x, n):
        scaled = (x.astype(F32) - stats[2 * n : 2 * n + 1]) * stats[2 * n + 1 : 2 * n + 2]
        scaled = scaled * gains[n : n + 1]
        return scaled * jax.nn.sigmoid(scaled)

    def turned(order, cells):
        return lax.dot_general(
            order, cells, (((1,), (1,)), ((), ())), preferred_element_type=F32
        ).astype(BF16)

    def activate_hidden():
        @pl.loop(0, T * H)
        def _(j):
            t, h = row_of(j)
            act[j, 0:W] = activated(hid[t, h], 1).astype(BF16)

        order = jnp.where(same, 1.0, 0.0).astype(BF16)
        act_t[...] = turned(order, act[...].reshape(T * H * WP, C))

    def activate_features():
        @pl.loop(0, 2 * T * (H + 2))
        def _(j):
            f, r = j // (H + 2), lax.rem(j, H + 2)
            inside = jnp.logical_and(
                jnp.logical_and(jnp.logical_or(r > 0, has_left), jnp.logical_or(r < H + 1, has_right)),
                jnp.logical_or(f >= T, has_before),
            )
            value = activated(wide_feat[f, r], 0)
            wide_act[f, r, 0:W] = jnp.where(inside, value, 0.0).astype(BF16)

        for b in range(3):
            cells = wide_act[:, b : b + H].reshape(2 * T * H * WP, C)
            wide_act_t[b] = turned(perm[...], cells)

    def own_row(ref, k):
        return ref[k : k + 1, pl.ds(off, half)]

    def centred_row(ref, n, t, h):
        x = ref[t, h, :, pl.ds(off, half)].astype(F32)
        return (x - own_row(stats, 2 * n)) * own_row(stats, 2 * n + 1)

    def slopes(ref, n):
        exchanged = 1 - n

        def row(j, carry):
            t, h = row_of(j)
            centred = centred_row(ref, n, t, h)
            scaled = centred * own_row(gains, n)
            gate = jax.nn.sigmoid(scaled)
            upstream = acc[ch, j, 0:W] + acc_in[exchanged, j, 0:W]
            value = upstream * gate * (1.0 + scaled * (1.0 - gate))
            slope[j, 0:W] = value
            return (
                carry[0] + jnp.sum(value, axis=0, keepdims=True),
                carry[1] + jnp.sum(value * centred, axis=0, keepdims=True),
            )

        zero = jnp.zeros((1, half), F32)
        return lax.fori_loop(0, T * H, row, (zero, zero))

    def norm_terms(n, totals):
        both = group_sum(totals * own_row(gains, n), half) * (1.0 / members)
        gg[n : n + 1] = totals[1:2]
        return both[0:1], both[1:2]

    def grad_row(ref, n, t, h, terms):
        first, second = terms
        centred = centred_row(ref, n, t, h)
        inner = slope[t * H + h, 0:W] * own_row(gains, n) - first - centred * second
        return own_row(stats, 2 * n + 1) * inner

    def hidden_rows(totals):
        terms = norm_terms(1, totals)

        @pl.loop(0, T * H)
        def _(j):
            t, h = row_of(j)
            graw1[t, h + 1] = grad_row(hid, 1, t, h, terms).astype(BF16)

    def feature_rows(totals):
        terms = norm_terms(0, totals)

        @pl.loop(0, T)
        def _(t):
            for h in range(H):
                base = graw2[t, h + 1].astype(F32)
                turn_half[t, :, h, :] = base + grad_row(feat, 0, t, h, terms)
            fgrad[t] = turn_half[t].astype(BF16)

    def by_rows(source, target):
        @pl.loop(0, T)
        def _(t):
            turn[...] = source[t].astype(F32)
            for h in range(H):
                target[t, h] = turn[:, h, :].astype(BF16)

    def reduce_slopes(n, parts):
        for k in range(2):
            zb_b[n, tm, k : k + 1] = parts[k]
        along_z(2 - n, zb_b.at[n])

    along_z(0, zb_a)
    halo_start(0, graw2)
    tmp[...] = jnp.zeros_like(tmp)
    act[...] = jnp.zeros_like(act)
    wide_act[...] = jnp.zeros_like(wide_act)
    for graw in (graw2, graw1):
        @pl.when(sp == 0)
        def _():
            graw[:, 0] = jnp.zeros((2 * T, W, half), BF16)

        @pl.when(sp == NS - 1)
        def _():
            graw[:, H + 1] = jnp.zeros((2 * T, W, half), BF16)

        @pl.when(tm == NT - 1)
        def _():
            graw[T : 2 * T] = jnp.zeros((T, H + 2, W, half), BF16)

    rows = lax.broadcasted_iota(jnp.int32, (C, C), 0)
    cols = lax.broadcasted_iota(jnp.int32, (C, C), 1)
    within = lax.rem(rows, R)
    source = within // share * (NS * share) + rows // R * share + lax.rem(within, share)
    perm[...] = jnp.where(cols == source, 1.0, 0.0).astype(BF16)
    same = rows == cols
    block_sum[...] = jnp.where(rows // per == cols // per, 1.0, 0.0).astype(F32)
    by_rows(feat_n, feat)
    feature_start()
    by_rows(hid_n, hid)

    def back_parts(kernel, later):
        for f in range(T):
            for a in (2, 1, 0):
                if (f + 2 - a >= T) == later:
                    back_part(kernel, f, a, a == 2)

    halo_wait(0, graw2, (0, 1))
    shift(graw2, 0, T)
    loads[3].wait()
    back_parts(k2, False)
    z_to_x(0, zb_a, xb_a)
    halo_wait(0, graw2, (2, 3, 4))
    shift(graw2, T, 2 * T)
    back_parts(k2, True)
    exchange(0).start()
    totals = lax.dot_general(
        x_total(0, zb_a, xb_a), spread_sum[...], (((1,), (1,)), ((), ())),
        precision=lax.Precision.HIGHEST, preferred_element_type=F32,
    ) * (1.0 / members)
    for n in range(2):
        mean = totals[2 * n : 2 * n + 1]
        spread = totals[2 * n + 1 : 2 * n + 2] - mean * mean
        stats[2 * n : 2 * n + 1] = mean
        stats[2 * n + 1 : 2 * n + 2] = lax.rsqrt(spread + EPS)
    exchange(0).wait_recv()
    reduce_slopes(1, slopes(hid, 1))
    activate_hidden()
    for p in range(3):
        delta_part(p)
        tick(p, 0, 0)
        tick(p, 1, 0)
    feature_wait()
    activate_features()
    z_to_x(1, zb_b.at[1], xb_b.at[1])
    ticks(0, 1)
    ticks(1, 1)
    totals_two = x_total(1, zb_b.at[1], xb_b.at[1])

    hidden_rows(totals_two)
    halo_start(1, graw1)
    shift_own(graw1)
    for p in range(3, 8):
        delta_part(p)
        rs_start(p)
        if p == 3:
            ticks(0, 2)
            ticks(1, 2)
    loads[4].wait()
    exchange(0).wait_send()
    halo_wait(1, graw1, (0, 1))
    shift_edges(graw1)
    ticks(0, 3)
    back_parts(k1, False)
    for p in range(3, 8):
        rs_pass(p)
    halo_wait(1, graw1, (2, 3, 4))
    ticks(0, 4)
    shift(graw1, T, 2 * T)
    back_parts(k1, True)
    exchange(1).start()
    ticks(1, 3)
    ticks(0, 5)
    rs_z1(3)
    exchange(1).wait_recv()
    reduce_slopes(0, slopes(feat, 0))
    ticks(1, 4)
    ticks(0, 6)
    rs_z1(4)
    rs_z2(3)
    ticks(1, 5)
    for p in range(5, 8):
        rs_z1(p)
    ticks(0, 7)
    rs_z2(4)
    z_to_x(2, zb_b.at[0], xb_b.at[0])
    ticks(1, 6)
    for p in range(5, 8):
        rs_z2(p)
    feature_rows(x_total(2, zb_b.at[0], xb_b.at[0]))
    for q in range(3):
        ring_pass(q)
    for p in range(3, 8):
        rs_end(p)
    for q in range(3):
        ring_end(q)

    halo_sent(0, graw2)
    halo_sent(1, graw1)
    feature_sent()
    reduced_sent(0, zb_a, xb_a)
    reduced_sent(1, zb_b.at[1], xb_b.at[1])
    reduced_sent(2, zb_b.at[0], xb_b.at[0])
    exchange(1).wait_send()
    for p in range(3, 8):
        rs_sent(p)
    for q in range(3):
        ring_sent(q)


def hand_on(*refs):
    count = len(refs) // 2
    for source, target in zip(refs[:count], refs[count:]):
        target[...] = source[...]


def shards(features, hidden, cotangent, kernel_one, kernel_two, gains):
    T, H, W, C = features.shape
    half = kernel_one.shape[4]
    NT, NS = lax.axis_size("tm"), lax.axis_size("space")
    share = C // (NT * NS)
    R = NT * share
    WP = padded_width(W)
    wide = 9 * half

    def by_tap(kernel):
        return jnp.transpose(kernel, (1, 2, 3, 0, 4)).reshape(27, C, half)

    vmem = pl.BlockSpec(memory_space=pltpu.VMEM)
    hbm = pl.BlockSpec(memory_space=pl.ANY)
    DMA = pltpu.SemaphoreType.DMA
    call = pl.pallas_call(
        functools.partial(body, (T, H, W, C, half, NT, NS)),
        out_shape=(
            jax.ShapeDtypeStruct((T, W, H, half), BF16),
            jax.ShapeDtypeStruct((27, share, half), F32),
            jax.ShapeDtypeStruct((27, share, half), F32),
            jax.ShapeDtypeStruct((2, half), F32),
        ),
        in_specs=[hbm] * 5 + [vmem],
        out_specs=(vmem,) * 4,
        scratch_shapes=[
            pltpu.VMEM((T, W, H, C), BF16),
            pltpu.VMEM((T, W, H, C), BF16),
            pltpu.VMEM((T, W, H, C), BF16),
            pltpu.VMEM((2 * T, H + 2, W, C), BF16),
            pltpu.VMEM((T, H, W, C), BF16),
            pltpu.VMEM((27, C, half), BF16),
            pltpu.VMEM((27, C, half), BF16),
            pltpu.VMEM((2 * T, H + 2, W, half), BF16),
            pltpu.VMEM((2 * T, H + 2, W, half), BF16),
            pltpu.VMEM((W, H, C), F32),
            pltpu.VMEM((T, W, H, half), F32),
            pltpu.VMEM((WP + 16, half), F32),
            pltpu.VMEM((2 * T, H + 2, WP, 3 * half), BF16),
            pltpu.VMEM((T * H, WP, C), BF16),
            pltpu.VMEM((C, T * H * WP), BF16),
            pltpu.VMEM((2 * T, H + 2, WP, C), BF16),
            pltpu.VMEM((3, C, 2 * T * H * WP), BF16),
            pltpu.VMEM((3, C, wide), F32),
            pltpu.VMEM((C, C), BF16),
            pltpu.VMEM((C, C), F32),
            pltpu.VMEM((C, half), F32),
            pltpu.VMEM((2, T * H, WP, half), F32),
            pltpu.VMEM((2, T * H, WP, half), F32),
            pltpu.VMEM((T * H, WP, half), F32),
            pltpu.VMEM((8, C), F32),
            pltpu.VMEM((NT, 4, half), F32),
            pltpu.VMEM((NS, 4, half), F32),
            pltpu.VMEM((2, NT, 2, half), F32),
            pltpu.VMEM((2, NS, 2, half), F32),
            pltpu.VMEM((6, C, wide), BF16),
            pltpu.VMEM((6, 2, R // 2, wide), BF16),
            pltpu.VMEM((6, 2, R, wide), BF16),
            pltpu.VMEM((R, wide), F32),
            pltpu.VMEM((6, 2, NT // 2, share, wide), F32),
            pltpu.VMEM((6, 2, NT // 2, share, wide), BF16),
            pltpu.VMEM((6, NT // 2, share, wide), BF16),
            pltpu.VMEM((6, NT // 2, share, wide), BF16),
            pltpu.VMEM((6, NT // 2 - 1, share, wide), BF16),
            pltpu.VMEM((3, NT - 1, NS * share, wide), BF16),
            pltpu.VMEM((3, NS, share, wide), F32),
            pltpu.VMEM((3, NS, share, wide), BF16),
            pltpu.VMEM((3, NS - 1, share, wide), BF16),
            DMA((5,)),
            DMA((3, 5)),
            DMA((3, 5)),
            DMA((3, 2)),
            DMA((3, 2)),
            DMA((2,)),
            DMA((2,)),
            DMA((8, 2)),
            DMA((8, 2)),
            DMA((8, 2)),
            DMA((8, 2)),
            DMA((8,)),
            DMA((8,)),
            DMA((8,)),
            DMA((8,)),
            DMA((3, NT - 1)),
            DMA((3, NT - 1)),
            DMA((3, NS - 1)),
            DMA((3, NS - 1)),
        ],
        compiler_params=pltpu.CompilerParams(
            collective_id=0, has_side_effects=True, vmem_limit_bytes=60 * 1024 * 1024
        ),
        name="block_back",
    )
    def by_column(field):
        return jnp.transpose(field, (0, 2, 1, 3))

    made = call(
        by_column(features), by_column(hidden), by_column(cotangent),
        by_tap(kernel_one), by_tap(kernel_two), gains,
    )
    fgrad, d1, d2, gg = pl.pallas_call(
        hand_on,
        out_shape=tuple(jax.ShapeDtypeStruct(x.shape, x.dtype) for x in made),
        in_specs=[vmem] * 4,
        out_specs=(vmem,) * 4,
        name="hand_on",
    )(*made)

    def by_channel(delta):
        return jnp.transpose(delta.reshape(3, 3, 3, share, half), (3, 0, 1, 2, 4))

    return (by_column(fgrad), by_channel(d1), by_channel(d2), gg)


def solution(mesh):
    placed = (
        P(("clip", "tm"), "space", None, None),
        P(("clip", "tm"), "space", None, None),
        P(("clip", "tm"), "space", None, None),
        P(None, None, None, None, "chan"),
        P(None, None, None, None, "chan"),
        P(),
    )
    return jax.shard_map(
        shards,
        mesh=mesh,
        in_specs=placed,
        out_specs=(
            P(("clip", "tm"), "space", None, "chan"),
            P(("clip", "tm", "space"), None, None, None, "chan"),
            P(("clip", "tm", "space"), None, None, None, "chan"),
            P("clip", "chan"),
        ),
        check_vma=False,
    )
```

```python
import functools

import jax
import jax.numpy as jnp
from jax import lax
from jax.experimental import pallas as pl
from jax.experimental.pallas import tpu as pltpu
from jax.sharding import PartitionSpec as P

GROUPS = 32
PIECES = ((0, 0, 3), (1, 0, 3), (2, 0, 3), (3, 0, 3), (4, 0, 3), (5, 0, 1), (5, 1, 2), (5, 2, 3))
EPS = 1e-06
MESH = pl.DeviceIdType.MESH
F32 = jnp.float32
BF16 = jnp.bfloat16


def padded_width(width):
    return (width + 2 + 15) // 16 * 16


def body(
    dims,
    feat_hbm, hid_hbm, cot_hbm, k1_hbm, k2_hbm, gains,
    fgrad, d1, d2, gg,
    feat_n, hid_n, cot_n, wide_feat, hid, k1, k2,
    graw2, graw1, turn, turn_half, tmp, ext, act, act_t, wide_act, wide_act_t, own_f, perm, block_sum, spread_sum,
    acc, acc_in, slope, stats,
    zb_a, xb_a, zb_b, xb_b,
    xs, xa, xb, zf, zk, zs, za, zc, zr, ring, ring_k, ring_s, ring_r,
    in_sem, halo_s, halo_r, ar_s, ar_r, ch_s, ch_r,
    xa_s, xa_r, xb_s, xb_r, za_s, za_r, z_s, z_r, hop_s, hop_r, last_s, last_r,
):
    T, H, W, C, half, NT, NS = dims
    WP = padded_width(W)
    per = C // GROUPS
    share = C // (NT * NS)
    R = NT * share
    members = float(T * H * W * per * NT * NS)
    tm, sp, ch = lax.axis_index("tm"), lax.axis_index("space"), lax.axis_index("chan")
    off = pl.multiple_of(ch * half, half)
    wide = 9 * half
    K3 = 3 * half
    feat = wide_feat.at[pl.ds(T, T), pl.ds(1, H)]

    def at_z(d):
        return lax.rem(tm + d, NT)

    def at_x(d):
        return lax.rem(sp + d, NS)

    def signal(barrier, where):
        pl.semaphore_signal(barrier, inc=1, device_id=where, device_id_type=MESH)

    def remote(src, dst, s, r, where):
        return pltpu.make_async_remote_copy(
            src_ref=src, dst_ref=dst, send_sem=s, recv_sem=r, device_id=where, device_id_type=MESH
        )

    loads = [
        pltpu.make_async_copy(src, dst, in_sem.at[i])
        for i, (src, dst) in enumerate(
            ((feat_hbm, feat_n), (hid_hbm, hid_n), (cot_hbm, cot_n), (k2_hbm, k2), (k1_hbm, k1))
        )
    ]
    for load in loads:
        load.start()

    barrier = pltpu.get_barrier_semaphore()

    @pl.loop(1, NT)
    def _(d):
        signal(barrier, {"tm": at_z(d)})

    for d in range(1, NS):
        signal(barrier, {"space": at_x(d)})
    signal(barrier, {"chan": 1 - ch})
    for dt in (1, NT - 1):
        for ds in (1, NS - 1):
            signal(barrier, {"tm": at_z(dt), "space": at_x(ds)})

    def group_sum(values, width):
        return lax.dot_general(
            values, block_sum[0:width, 0:width], (((1,), (0,)), ((), ())),
            precision=lax.Precision.HIGHEST, preferred_element_type=F32,
        )

    def row_of(j):
        return j // H, lax.rem(j, H)

    for load in loads[:3]:
        load.wait()

    rows = lax.broadcasted_iota(jnp.int32, (C, half), 0)
    cols = lax.broadcasted_iota(jnp.int32, (C, half), 1)
    spread_sum[...] = jnp.where(rows // per == cols, 1.0, 0.0).astype(F32)
    strip = W // 9 if W % 9 == 0 else 1

    def stat_strip(j, carry):
        t, w = j // (W // strip), lax.rem(j, W // strip) * strip
        out = []
        for k, ref in enumerate((feat_n, hid_n)):
            x = ref[t, pl.ds(w, strip)].astype(F32)
            out.append(carry[2 * k] + jnp.sum(x, axis=0))
            out.append(carry[2 * k + 1] + jnp.sum(x * x, axis=0))
        return tuple(out)

    sums = lax.fori_loop(0, T * (W // strip), stat_strip, (jnp.zeros((H, C), F32),) * 4)
    sums = jnp.concatenate([jnp.sum(x, axis=0, keepdims=True) for x in sums], axis=0)
    zb_a[tm] = lax.dot_general(
        sums, spread_sum[...], (((1,), (0,)), ((), ())),
        precision=lax.Precision.HIGHEST, preferred_element_type=F32,
    )
    for t in range(T):
        turn_half[t] = cot_n[t, :, :, pl.ds(off, half)].astype(F32)
        for h in range(H):
            graw2[t, h + 1] = turn_half[t, :, h, :].astype(BF16)
    pl.semaphore_wait(barrier, (NT - 1) + (NS - 1) + 1 + 4)

    def along_z(n, zb):
        @pl.loop(0, NT - 1)
        def _(k):
            step = (k + 1) // 2
            d = NT // 2 + jnp.where(lax.rem(k, 2) == 0, step, -step)
            remote(zb.at[tm], zb.at[tm], ar_s.at[n, 0], ar_r.at[n, 0], {"tm": at_z(d)}).start()

    def z_to_x(n, zb, xbuf):
        every = remote(
            zb.at[0 : NT - 1], zb.at[0 : NT - 1], ar_s.at[n, 0], ar_r.at[n, 0], {"tm": at_z(1)}
        )
        every.wait_recv()
        total = lax.fori_loop(1, NT, lambda j, c: c + zb[j], zb[0])
        xbuf[sp] = total
        for d in range(1, NS):
            remote(xbuf.at[sp], xbuf.at[sp], ar_s.at[n, 1], ar_r.at[n, 1], {"space": at_x(d)}).start()

    def x_total(n, zb, xbuf):
        last = remote(
            xbuf.at[0 : NS - 1], xbuf.at[0 : NS - 1], ar_s.at[n, 1], ar_r.at[n, 1], {"space": at_x(1)}
        )
        last.wait_recv()
        total = xbuf[0]
        for j in range(1, NS):
            total = total + xbuf[j]
        return total

    def reduced_sent(n, zb, xbuf):
        remote(
            zb.at[0 : NT - 1], zb.at[0 : NT - 1], ar_s.at[n, 0], ar_r.at[n, 0], {"tm": at_z(1)}
        ).wait_send()
        remote(
            xbuf.at[0 : NS - 1], xbuf.at[0 : NS - 1], ar_s.at[n, 1], ar_r.at[n, 1], {"space": at_x(1)}
        ).wait_send()

    def halo_copies(n, graw):
        right, left = at_x(1), at_x(NS - 1)
        before = at_z(NT - 1)
        own = pl.ds(0, T)
        later = pl.ds(T, T)
        plan = (
            (graw.at[own, H], graw.at[own, 0], {"space": right}),
            (graw.at[own, 1], graw.at[own, H + 1], {"space": left}),
            (graw.at[own, pl.ds(1, H)], graw.at[later, pl.ds(1, H)], {"tm": before}),
            (graw.at[own, H], graw.at[later, 0], {"tm": before, "space": right}),
            (graw.at[own, 1], graw.at[later, H + 1], {"tm": before, "space": left}),
        )
        return [
            remote(src, dst, halo_s.at[n, i], halo_r.at[n, i], where)
            for i, (src, dst, where) in enumerate(plan)
        ]

    has_right, has_left, has_before, has_after = sp < NS - 1, sp > 0, tm > 0, tm < NT - 1
    sends = (
        has_right,
        has_left,
        has_before,
        jnp.logical_and(has_before, has_right),
        jnp.logical_and(has_before, has_left),
    )
    arrives = (
        has_left,
        has_right,
        has_after,
        jnp.logical_and(has_after, has_left),
        jnp.logical_and(has_after, has_right),
    )

    def halo_start(n, graw):
        for copy, here in zip(halo_copies(n, graw), sends):
            @pl.when(here)
            def _():
                copy.start()

    def halo_wait(n, graw, which):
        copies = halo_copies(n, graw)
        for i in which:
            @pl.when(arrives[i])
            def _():
                copies[i].wait_recv()

    def halo_sent(n, graw):
        for copy, here in zip(halo_copies(n, graw), sends):
            @pl.when(here)
            def _():
                copy.wait_send()

    def feature_copies():
        right, left, after = at_x(1), at_x(NS - 1), at_z(1)
        own, earlier = pl.ds(T, T), pl.ds(0, T)
        w = wide_feat
        plan = (
            (w.at[own, H], w.at[own, 0], {"space": right}),
            (w.at[own, 1], w.at[own, H + 1], {"space": left}),
            (w.at[own, pl.ds(1, H)], w.at[earlier, pl.ds(1, H)], {"tm": after}),
            (w.at[own, H], w.at[earlier, 0], {"tm": after, "space": right}),
            (w.at[own, 1], w.at[earlier, H + 1], {"tm": after, "space": left}),
        )
        return [
            remote(src, dst, halo_s.at[2, i], halo_r.at[2, i], where)
            for i, (src, dst, where) in enumerate(plan)
        ]

    feature_sends = (
        has_right,
        has_left,
        has_after,
        jnp.logical_and(has_after, has_right),
        jnp.logical_and(has_after, has_left),
    )
    feature_arrives = (
        has_left,
        has_right,
        has_before,
        jnp.logical_and(has_before, has_left),
        jnp.logical_and(has_before, has_right),
    )

    def feature_start():
        for copy, here in zip(feature_copies(), feature_sends):
            @pl.when(here)
            def _():
                copy.start()

    def feature_wait():
        for copy, here in zip(feature_copies(), feature_arrives):
            @pl.when(here)
            def _():
                copy.wait_recv()

    def feature_sent():
        for copy, here in zip(feature_copies(), feature_sends):
            @pl.when(here)
            def _():
                copy.wait_send()

    def place_shifted(f, r, values):
        tmp[8 : 8 + W] = values
        for c in range(3):
            ext[f, r, :, c * half : (c + 1) * half] = tmp[9 - c : 9 - c + WP].astype(BF16)

    def shift(graw, first, last):
        @pl.loop(first * (H + 2), last * (H + 2))
        def _(j):
            f, r = j // (H + 2), lax.rem(j, H + 2)
            place_shifted(f, r, graw[f, r].astype(F32))

    def shift_own(graw):
        @pl.loop(0, T * H)
        def _(j):
            place_shifted(j // H, lax.rem(j, H) + 1, graw[j // H, lax.rem(j, H) + 1].astype(F32))

    def shift_edges(graw):
        @pl.loop(0, 2 * T)
        def _(j):
            f, r = j // 2, lax.rem(j, 2) * (H + 1)
            place_shifted(f, r, graw[f, r].astype(F32))

    def taps(f, a, b):
        return ext[f + 2 - a, 2 - b : 2 - b + H].reshape(H * WP, K3)

    def back_part(kernel, f, a, first):
        left = jnp.concatenate([taps(f, a, b) for b in range(3)], axis=1)
        right = jnp.concatenate([kernel[a * 9 + k] for k in range(9)], axis=1)
        product = lax.dot_general(left, right, (((1,), (1,)), ((), ())), preferred_element_type=F32)
        for k in range(2):
            piece = product[:, k * half : (k + 1) * half].reshape(H, WP, half)
            if first:
                acc[k, f * H : (f + 1) * H] = piece
            else:
                acc[k, f * H : (f + 1) * H] += piece

    def exchange(n):
        return remote(acc.at[1 - ch], acc_in.at[n], ch_s.at[n], ch_r.at[n], {"chan": 1 - ch})

    def lanes(p):
        q, low, high = PIECES[p]
        return q, pl.ds(low * K3, (high - low) * K3)

    def delta_part(p):
        q, low, high = PIECES[p]
        a = 2 - q % 3
        for b in range(low, high):
            if q < 3:
                left = act_t[...]
                right = jnp.concatenate([taps(f, a, b) for f in range(T)], axis=0)
            else:
                left = wide_act_t[b, :, a * H * WP : (a + T) * H * WP]
                right = jnp.concatenate([taps(f, 2, 1) for f in range(T)], axis=0)
            product = lax.dot_general(
                left, right, (((1,), (0,)), ((), ())), preferred_element_type=F32
            )
            xs[q, :, b * K3 : (b + 1) * K3] = product.astype(BF16)
            if q < 3:
                own_f[q, :, b * K3 : (b + 1) * K3] = product

    def chunk(s, part, parts):
        size = R // parts
        return pl.ds(pl.multiple_of(s * R + part * size, size), size)

    def sum_1(p):
        far = at_x(2)
        q, cut = lanes(p)
        return [
            remote(
                xs.at[q, chunk(far, k, 2), cut], xa.at[q, k, :, cut],
                xa_s.at[p, k], xa_r.at[p, k], {"space": at_x(d)},
            )
            for k, d in enumerate((1, NS - 1))
        ]

    def sum_2(p):
        q, cut = lanes(p)
        return [
            remote(
                xs.at[q, chunk(at_x(d), 0, 1), cut], xb.at[q, k, :, cut],
                xb_s.at[p, k], xb_r.at[p, k], {"space": at_x(d)},
            )
            for k, d in enumerate((1, NS - 1))
        ]

    def rs_start(p):
        for copy in sum_1(p):
            copy.start()

    def rs_pass(p):
        q, cut = lanes(p)
        for k, (first, second) in enumerate(zip(sum_1(p), sum_2(p))):
            first.wait_recv()
            rows = chunk(at_x((1, NS - 1)[k]), k, 2)
            xs[q, rows, cut] = (xs[q, rows, cut].astype(F32) + xa[q, k, :, cut].astype(F32)).astype(BF16)
            second.start()

    pairs = NT // 2
    parity = lax.rem(tm, 2)
    place = tm // 2

    def mate(p):
        turned = parity if p % 2 == 0 else 1 - parity
        return {"tm": lax.rem(tm + 1 - 2 * turned + NT, NT)}

    def to_mate(p):
        q, cut = lanes(p)
        return remote(
            zs.at[q, 1 - parity, :, :, cut], za.at[q, :, :, cut], za_s.at[p], za_r.at[p], mate(p)
        )

    def rs_z1(p):
        q, cut = lanes(p)
        for copy in sum_2(p):
            copy.wait_recv()
        kept = xs[q, chunk(sp, 0, 1), cut].astype(F32)
        zf[:, cut] = kept + xb[q, 0, :, cut].astype(F32) + xb[q, 1, :, cut].astype(F32)
        for t in range(NT):
            rows = zf[t * share : (t + 1) * share, cut]
            zk[q, t % 2, t // 2, :, cut] = rows
            zs[q, t % 2, t // 2, :, cut] = rows.astype(BF16)
        to_mate(p).start()

    def rs_z2(p):
        q, cut = lanes(p)
        to_mate(p).wait_recv()

        @pl.loop(0, pairs)
        def _(j):
            both = zk[q, parity, j, :, cut] + za[q, j, :, cut].astype(F32)
            zk[q, parity, j, :, cut] = both
            zc[q, j, :, cut] = both.astype(BF16)

        @pl.loop(1, pairs)
        def _(k):
            d = lax.rem(k + pairs // 2 - 1, pairs - 1) + 1
            to = lax.rem(place + d, pairs)
            remote(
                zc.at[q, to, :, cut], zr.at[q, d - 1, :, cut], z_s.at[p], z_r.at[p],
                {"tm": 2 * to + parity},
            ).start()

    def z_all(p):
        q, cut = lanes(p)
        return remote(
            zc.at[q, pl.ds(0, pairs - 1), :, cut], zr.at[q, :, :, cut], z_s.at[p], z_r.at[p], mate(p)
        )

    def rs_end(p):
        q, low, high = PIECES[p]
        cut = lanes(p)[1]
        z_all(p).wait_recv()
        total = zk[q, parity, place, :, cut]
        for j in range(pairs - 1):
            total = total + zr[q, j, :, cut].astype(F32)
        out, a = (d2, d1)[q // 3], 2 - q % 3
        for k in range(3 * (high - low)):
            out[a * 9 + 3 * low + k] = total[:, k * half : (k + 1) * half]

    def rs_sent(p):
        for copy in sum_1(p) + sum_2(p):
            copy.wait_send()
        to_mate(p).wait_send()
        z_all(p).wait_send()

    steps = (NT // 2, NT - 1 - NT // 2)
    band = NS * share

    def band_of(t):
        return pl.ds(pl.multiple_of(t * band, band), band)

    def hop(q, way, k):
        if way == 0:
            dest, to, slot = at_z(steps[0] - k), at_z(1), k
        else:
            dest, to, slot = at_z(NT - steps[1] + k), at_z(NT - 1), steps[0] + k
        return dest, remote(
            xs.at[q, band_of(dest)], ring.at[q, slot], hop_s.at[q, slot], hop_r.at[q, slot], {"tm": to}
        )

    def tick(q, way, k):
        dest, copy = hop(q, way, k)
        if k > 0:
            hop(q, way, k - 1)[1].wait_recv()
            came = ring[q, way * steps[0] + k - 1].astype(F32)
            xs[q, band_of(dest)] = (own_f[q, band_of(dest)] + came).astype(BF16)
        copy.start()

    def ticks(way, k):
        for q in range(3):
            tick(q, way, k)

    def across(q, d):
        return remote(
            ring_s.at[q, at_x(d)], ring_r.at[q, d - 1], last_s.at[q, d - 1], last_r.at[q, d - 1],
            {"space": at_x(d)},
        )

    def ring_pass(q):
        for way in range(2):
            hop(q, way, steps[way] - 1)[1].wait_recv()
        total = own_f[q, band_of(tm)]
        total = total + ring[q, steps[0] - 1].astype(F32) + ring[q, NT - 2].astype(F32)
        zf[0:band] = total
        for x in range(NS):
            rows = zf[x * share : (x + 1) * share]
            ring_k[q, x] = rows
            ring_s[q, x] = rows.astype(BF16)
        for d in range(1, NS):
            across(q, d).start()

    def ring_end(q):
        total = ring_k[q, sp]
        for d in range(1, NS):
            across(q, d).wait_recv()
            total = total + ring_r[q, d - 1].astype(F32)
        for k in range(9):
            d2[(2 - q) * 9 + k] = total[:, k * half : (k + 1) * half]

    def ring_sent(q):
        for way in range(2):
            for k in range(steps[way]):
                hop(q, way, k)[1].wait_send()
        for d in range(1, NS):
            across(q, d).wait_send()

    def activated(x, n):
        scaled = (x.astype(F32) - stats[2 * n : 2 * n + 1]) * stats[2 * n + 1 : 2 * n + 2]
        scaled = scaled * gains[n : n + 1]
        return scaled * jax.nn.sigmoid(scaled)

    def turned(order, cells):
        return lax.dot_general(
            order, cells, (((1,), (1,)), ((), ())), preferred_element_type=F32
        ).astype(BF16)

    def activate_hidden():
        @pl.loop(0, T * H)
        def _(j):
            t, h = row_of(j)
            act[j, 0:W] = activated(hid[t, h], 1).astype(BF16)

        order = jnp.where(same, 1.0, 0.0).astype(BF16)
        act_t[...] = turned(order, act[...].reshape(T * H * WP, C))

    def activate_features():
        @pl.loop(0, 2 * T * (H + 2))
        def _(j):
            f, r = j // (H + 2), lax.rem(j, H + 2)
            inside = jnp.logical_and(
                jnp.logical_and(jnp.logical_or(r > 0, has_left), jnp.logical_or(r < H + 1, has_right)),
                jnp.logical_or(f >= T, has_before),
            )
            value = activated(wide_feat[f, r], 0)
            wide_act[f, r, 0:W] = jnp.where(inside, value, 0.0).astype(BF16)

        for b in range(3):
            cells = wide_act[:, b : b + H].reshape(2 * T * H * WP, C)
            wide_act_t[b] = turned(perm[...], cells)

    def own_row(ref, k):
        return ref[k : k + 1, pl.ds(off, half)]

    def centred_row(ref, n, t, h):
        x = ref[t, h, :, pl.ds(off, half)].astype(F32)
        return (x - own_row(stats, 2 * n)) * own_row(stats, 2 * n + 1)

    def slopes(ref, n):
        exchanged = 1 - n

        def row(j, carry):
            t, h = row_of(j)
            centred = centred_row(ref, n, t, h)
            scaled = centred * own_row(gains, n)
            gate = jax.nn.sigmoid(scaled)
            upstream = acc[ch, j, 0:W] + acc_in[exchanged, j, 0:W]
            value = upstream * gate * (1.0 + scaled * (1.0 - gate))
            slope[j, 0:W] = value
            return (
                carry[0] + jnp.sum(value, axis=0, keepdims=True),
                carry[1] + jnp.sum(value * centred, axis=0, keepdims=True),
            )

        zero = jnp.zeros((1, half), F32)
        return lax.fori_loop(0, T * H, row, (zero, zero))

    def norm_terms(n, totals):
        both = group_sum(totals * own_row(gains, n), half) * (1.0 / members)
        gg[n : n + 1] = totals[1:2]
        return both[0:1], both[1:2]

    def grad_row(ref, n, t, h, terms):
        first, second = terms
        centred = centred_row(ref, n, t, h)
        inner = slope[t * H + h, 0:W] * own_row(gains, n) - first - centred * second
        return own_row(stats, 2 * n + 1) * inner

    def hidden_rows(totals):
        terms = norm_terms(1, totals)

        @pl.loop(0, T * H)
        def _(j):
            t, h = row_of(j)
            graw1[t, h + 1] = grad_row(hid, 1, t, h, terms).astype(BF16)

    def feature_rows(totals):
        terms = norm_terms(0, totals)

        @pl.loop(0, T)
        def _(t):
            for h in range(H):
                base = graw2[t, h + 1].astype(F32)
                turn_half[t, :, h, :] = base + grad_row(feat, 0, t, h, terms)
            fgrad[t] = turn_half[t].astype(BF16)

    def by_rows(source, target):
        @pl.loop(0, T)
        def _(t):
            turn[...] = source[t].astype(F32)
            for h in range(H):
                target[t, h] = turn[:, h, :].astype(BF16)

    def reduce_slopes(n, parts):
        for k in range(2):
            zb_b[n, tm, k : k + 1] = parts[k]
        along_z(2 - n, zb_b.at[n])

    along_z(0, zb_a)
    halo_start(0, graw2)
    tmp[...] = jnp.zeros_like(tmp)
    act[...] = jnp.zeros_like(act)
    wide_act[...] = jnp.zeros_like(wide_act)
    for graw in (graw2, graw1):
        @pl.when(sp == 0)
        def _():
            graw[:, 0] = jnp.zeros((2 * T, W, half), BF16)

        @pl.when(sp == NS - 1)
        def _():
            graw[:, H + 1] = jnp.zeros((2 * T, W, half), BF16)

        @pl.when(tm == NT - 1)
        def _():
            graw[T : 2 * T] = jnp.zeros((T, H + 2, W, half), BF16)

    rows = lax.broadcasted_iota(jnp.int32, (C, C), 0)
    cols = lax.broadcasted_iota(jnp.int32, (C, C), 1)
    within = lax.rem(rows, R)
    source = within // share * (NS * share) + rows // R * share + lax.rem(within, share)
    perm[...] = jnp.where(cols == source, 1.0, 0.0).astype(BF16)
    same = rows == cols
    block_sum[...] = jnp.where(rows // per == cols // per, 1.0, 0.0).astype(F32)
    by_rows(feat_n, feat)
    feature_start()
    by_rows(hid_n, hid)

    def back_parts(kernel, later):
        for f in range(T):
            for a in (2, 1, 0):
                if (f + 2 - a >= T) == later:
                    back_part(kernel, f, a, a == 2)

    halo_wait(0, graw2, (0, 1))
    shift(graw2, 0, T)
    loads[3].wait()
    back_parts(k2, False)
    z_to_x(0, zb_a, xb_a)
    halo_wait(0, graw2, (2, 3, 4))
    shift(graw2, T, 2 * T)
    back_parts(k2, True)
    exchange(0).start()
    totals = lax.dot_general(
        x_total(0, zb_a, xb_a), spread_sum[...], (((1,), (1,)), ((), ())),
        precision=lax.Precision.HIGHEST, preferred_element_type=F32,
    ) * (1.0 / members)
    for n in range(2):
        mean = totals[2 * n : 2 * n + 1]
        spread = totals[2 * n + 1 : 2 * n + 2] - mean * mean
        stats[2 * n : 2 * n + 1] = mean
        stats[2 * n + 1 : 2 * n + 2] = lax.rsqrt(spread + EPS)
    exchange(0).wait_recv()
    reduce_slopes(1, slopes(hid, 1))
    activate_hidden()
    for p in range(3):
        delta_part(p)
        tick(p, 0, 0)
        tick(p, 1, 0)
    feature_wait()
    activate_features()
    z_to_x(1, zb_b.at[1], xb_b.at[1])
    ticks(0, 1)
    ticks(1, 1)
    totals_two = x_total(1, zb_b.at[1], xb_b.at[1])

    hidden_rows(totals_two)
    halo_start(1, graw1)
    shift_own(graw1)
    for p in range(3, 8):
        delta_part(p)
        rs_start(p)
        if p == 3:
            ticks(0, 2)
            ticks(1, 2)
    loads[4].wait()
    exchange(0).wait_send()
    halo_wait(1, graw1, (0, 1))
    shift_edges(graw1)
    back_parts(k1, False)
    rs_pass(3)
    ticks(0, 3)
    for p in range(4, 8):
        rs_pass(p)
    halo_wait(1, graw1, (2, 3, 4))
    ticks(0, 4)
    ticks(1, 3)
    shift(graw1, T, 2 * T)
    back_parts(k1, True)
    exchange(1).start()
    rs_z1(3)
    ticks(0, 5)
    ticks(1, 4)
    exchange(1).wait_recv()
    reduce_slopes(0, slopes(feat, 0))
    rs_z1(4)
    ticks(0, 6)
    ticks(1, 5)
    rs_z2(3)
    for p in range(5, 8):
        rs_z1(p)
    ticks(0, 7)
    ticks(1, 6)
    rs_z2(4)
    for p in range(5, 8):
        rs_z2(p)
    z_to_x(2, zb_b.at[0], xb_b.at[0])
    for q in range(3):
        ring_pass(q)
    feature_rows(x_total(2, zb_b.at[0], xb_b.at[0]))
    for q in range(3):
        ring_end(q)
    for p in range(3, 8):
        rs_end(p)

    halo_sent(0, graw2)
    halo_sent(1, graw1)
    feature_sent()
    reduced_sent(0, zb_a, xb_a)
    reduced_sent(1, zb_b.at[1], xb_b.at[1])
    reduced_sent(2, zb_b.at[0], xb_b.at[0])
    exchange(1).wait_send()
    for p in range(3, 8):
        rs_sent(p)
    for q in range(3):
        ring_sent(q)


def hand_on(*refs):
    count = len(refs) // 2
    for source, target in zip(refs[:count], refs[count:]):
        target[...] = source[...]


def shards(features, hidden, cotangent, kernel_one, kernel_two, gains):
    T, H, W, C = features.shape
    half = kernel_one.shape[4]
    NT, NS = lax.axis_size("tm"), lax.axis_size("space")
    share = C // (NT * NS)
    R = NT * share
    WP = padded_width(W)
    wide = 9 * half

    def by_tap(kernel):
        return jnp.transpose(kernel, (1, 2, 3, 0, 4)).reshape(27, C, half)

    vmem = pl.BlockSpec(memory_space=pltpu.VMEM)
    hbm = pl.BlockSpec(memory_space=pl.ANY)
    DMA = pltpu.SemaphoreType.DMA
    call = pl.pallas_call(
        functools.partial(body, (T, H, W, C, half, NT, NS)),
        out_shape=(
            jax.ShapeDtypeStruct((T, W, H, half), BF16),
            jax.ShapeDtypeStruct((27, share, half), F32),
            jax.ShapeDtypeStruct((27, share, half), F32),
            jax.ShapeDtypeStruct((2, half), F32),
        ),
        in_specs=[hbm] * 5 + [vmem],
        out_specs=(vmem,) * 4,
        scratch_shapes=[
            pltpu.VMEM((T, W, H, C), BF16),
            pltpu.VMEM((T, W, H, C), BF16),
            pltpu.VMEM((T, W, H, C), BF16),
            pltpu.VMEM((2 * T, H + 2, W, C), BF16),
            pltpu.VMEM((T, H, W, C), BF16),
            pltpu.VMEM((27, C, half), BF16),
            pltpu.VMEM((27, C, half), BF16),
            pltpu.VMEM((2 * T, H + 2, W, half), BF16),
            pltpu.VMEM((2 * T, H + 2, W, half), BF16),
            pltpu.VMEM((W, H, C), F32),
            pltpu.VMEM((T, W, H, half), F32),
            pltpu.VMEM((WP + 16, half), F32),
            pltpu.VMEM((2 * T, H + 2, WP, 3 * half), BF16),
            pltpu.VMEM((T * H, WP, C), BF16),
            pltpu.VMEM((C, T * H * WP), BF16),
            pltpu.VMEM((2 * T, H + 2, WP, C), BF16),
            pltpu.VMEM((3, C, 2 * T * H * WP), BF16),
            pltpu.VMEM((3, C, wide), F32),
            pltpu.VMEM((C, C), BF16),
            pltpu.VMEM((C, C), F32),
            pltpu.VMEM((C, half), F32),
            pltpu.VMEM((2, T * H, WP, half), F32),
            pltpu.VMEM((2, T * H, WP, half), F32),
            pltpu.VMEM((T * H, WP, half), F32),
            pltpu.VMEM((8, C), F32),
            pltpu.VMEM((NT, 4, half), F32),
            pltpu.VMEM((NS, 4, half), F32),
            pltpu.VMEM((2, NT, 2, half), F32),
            pltpu.VMEM((2, NS, 2, half), F32),
            pltpu.VMEM((6, C, wide), BF16),
            pltpu.VMEM((6, 2, R // 2, wide), BF16),
            pltpu.VMEM((6, 2, R, wide), BF16),
            pltpu.VMEM((R, wide), F32),
            pltpu.VMEM((6, 2, NT // 2, share, wide), F32),
            pltpu.VMEM((6, 2, NT // 2, share, wide), BF16),
            pltpu.VMEM((6, NT // 2, share, wide), BF16),
            pltpu.VMEM((6, NT // 2, share, wide), BF16),
            pltpu.VMEM((6, NT // 2 - 1, share, wide), BF16),
            pltpu.VMEM((3, NT - 1, NS * share, wide), BF16),
            pltpu.VMEM((3, NS, share, wide), F32),
            pltpu.VMEM((3, NS, share, wide), BF16),
            pltpu.VMEM((3, NS - 1, share, wide), BF16),
            DMA((5,)),
            DMA((3, 5)),
            DMA((3, 5)),
            DMA((3, 2)),
            DMA((3, 2)),
            DMA((2,)),
            DMA((2,)),
            DMA((8, 2)),
            DMA((8, 2)),
            DMA((8, 2)),
            DMA((8, 2)),
            DMA((8,)),
            DMA((8,)),
            DMA((8,)),
            DMA((8,)),
            DMA((3, NT - 1)),
            DMA((3, NT - 1)),
            DMA((3, NS - 1)),
            DMA((3, NS - 1)),
        ],
        compiler_params=pltpu.CompilerParams(
            collective_id=0, has_side_effects=True, vmem_limit_bytes=60 * 1024 * 1024
        ),
        name="block_back",
    )
    def by_column(field):
        return jnp.transpose(field, (0, 2, 1, 3))

    made = call(
        by_column(features), by_column(hidden), by_column(cotangent),
        by_tap(kernel_one), by_tap(kernel_two), gains,
    )
    fgrad, d1, d2, gg = pl.pallas_call(
        hand_on,
        out_shape=tuple(jax.ShapeDtypeStruct(x.shape, x.dtype) for x in made),
        in_specs=[vmem] * 4,
        out_specs=(vmem,) * 4,
        name="hand_on",
    )(*made)

    def by_channel(delta):
        return jnp.transpose(delta.reshape(3, 3, 3, share, half), (3, 0, 1, 2, 4))

    return (by_column(fgrad), by_channel(d1), by_channel(d2), gg)


def solution(mesh):
    placed = (
        P(("clip", "tm"), "space", None, None),
        P(("clip", "tm"), "space", None, None),
        P(("clip", "tm"), "space", None, None),
        P(None, None, None, None, "chan"),
        P(None, None, None, None, "chan"),
        P(),
    )
    return jax.shard_map(
        shards,
        mesh=mesh,
        in_specs=placed,
        out_specs=(
            P(("clip", "tm"), "space", None, "chan"),
            P(("clip", "tm", "space"), None, None, None, "chan"),
            P(("clip", "tm", "space"), None, None, None, "chan"),
            P("clip", "chan"),
        ),
        check_vma=False,
    )
```

```python
import functools

import jax
import jax.numpy as jnp
from jax import lax
from jax.experimental import pallas as pl
from jax.experimental.pallas import tpu as pltpu
from jax.sharding import PartitionSpec as P

GROUPS = 32
PIECES = ((0, 0, 3), (1, 0, 3), (2, 0, 3), (3, 0, 3), (4, 0, 3), (5, 0, 1), (5, 1, 2), (5, 2, 3))
EPS = 1e-06
MESH = pl.DeviceIdType.MESH
F32 = jnp.float32
BF16 = jnp.bfloat16


def padded_width(width):
    return (width + 2 + 15) // 16 * 16


def body(
    dims,
    feat_hbm, hid_hbm, cot_hbm, k1_hbm, k2_hbm, gains,
    fgrad, d1, d2, gg,
    feat_n, hid_n, cot_n, wide_feat, hid, k1, k2,
    graw2, graw1, turn, turn_half, tmp, ext, act, act_t, wide_act, wide_act_t, own_f, perm, block_sum, spread_sum,
    acc, acc_in, slope, stats,
    zb_a, xb_a, zb_b, xb_b,
    xs, xa, xb, zf, zk, zs, za, zc, zr, ring, ring_k, ring_s, ring_r,
    in_sem, halo_s, halo_r, ar_s, ar_r, ch_s, ch_r,
    xa_s, xa_r, xb_s, xb_r, za_s, za_r, z_s, z_r, hop_s, hop_r, last_s, last_r,
):
    T, H, W, C, half, NT, NS = dims
    WP = padded_width(W)
    per = C // GROUPS
    share = C // (NT * NS)
    R = NT * share
    members = float(T * H * W * per * NT * NS)
    tm, sp, ch = lax.axis_index("tm"), lax.axis_index("space"), lax.axis_index("chan")
    off = pl.multiple_of(ch * half, half)
    wide = 9 * half
    K3 = 3 * half
    feat = wide_feat.at[pl.ds(T, T), pl.ds(1, H)]

    def at_z(d):
        return lax.rem(tm + d, NT)

    def at_x(d):
        return lax.rem(sp + d, NS)

    def signal(barrier, where):
        pl.semaphore_signal(barrier, inc=1, device_id=where, device_id_type=MESH)

    def remote(src, dst, s, r, where):
        return pltpu.make_async_remote_copy(
            src_ref=src, dst_ref=dst, send_sem=s, recv_sem=r, device_id=where, device_id_type=MESH
        )

    loads = [
        pltpu.make_async_copy(src, dst, in_sem.at[i])
        for i, (src, dst) in enumerate(
            ((feat_hbm, feat_n), (hid_hbm, hid_n), (cot_hbm, cot_n), (k2_hbm, k2), (k1_hbm, k1))
        )
    ]
    for load in loads:
        load.start()

    barrier = pltpu.get_barrier_semaphore()

    @pl.loop(1, NT)
    def _(d):
        signal(barrier, {"tm": at_z(d)})

    for d in range(1, NS):
        signal(barrier, {"space": at_x(d)})
    signal(barrier, {"chan": 1 - ch})
    for dt in (1, NT - 1):
        for ds in (1, NS - 1):
            signal(barrier, {"tm": at_z(dt), "space": at_x(ds)})

    def group_sum(values, width):
        return lax.dot_general(
            values, block_sum[0:width, 0:width], (((1,), (0,)), ((), ())),
            precision=lax.Precision.HIGHEST, preferred_element_type=F32,
        )

    def row_of(j):
        return j // H, lax.rem(j, H)

    for load in loads[:3]:
        load.wait()

    rows = lax.broadcasted_iota(jnp.int32, (C, half), 0)
    cols = lax.broadcasted_iota(jnp.int32, (C, half), 1)
    spread_sum[...] = jnp.where(rows // per == cols, 1.0, 0.0).astype(F32)
    strip = W // 9 if W % 9 == 0 else 1

    def stat_strip(j, carry):
        t, w = j // (W // strip), lax.rem(j, W // strip) * strip
        out = []
        for k, ref in enumerate((feat_n, hid_n)):
            x = ref[t, pl.ds(w, strip)].astype(F32)
            out.append(carry[2 * k] + jnp.sum(x, axis=0))
            out.append(carry[2 * k + 1] + jnp.sum(x * x, axis=0))
        return tuple(out)

    sums = lax.fori_loop(0, T * (W // strip), stat_strip, (jnp.zeros((H, C), F32),) * 4)
    sums = jnp.concatenate([jnp.sum(x, axis=0, keepdims=True) for x in sums], axis=0)
    zb_a[tm] = lax.dot_general(
        sums, spread_sum[...], (((1,), (0,)), ((), ())),
        precision=lax.Precision.HIGHEST, preferred_element_type=F32,
    )
    for t in range(T):
        turn_half[t] = cot_n[t, :, :, pl.ds(off, half)].astype(F32)
        for h in range(H):
            graw2[t, h + 1] = turn_half[t, :, h, :].astype(BF16)
    pl.semaphore_wait(barrier, (NT - 1) + (NS - 1) + 1 + 4)

    def along_z(n, zb):
        @pl.loop(0, NT - 1)
        def _(k):
            step = (k + 1) // 2
            d = NT // 2 + jnp.where(lax.rem(k, 2) == 0, step, -step)
            remote(zb.at[tm], zb.at[tm], ar_s.at[n, 0], ar_r.at[n, 0], {"tm": at_z(d)}).start()

    def z_to_x(n, zb, xbuf):
        every = remote(
            zb.at[0 : NT - 1], zb.at[0 : NT - 1], ar_s.at[n, 0], ar_r.at[n, 0], {"tm": at_z(1)}
        )
        every.wait_recv()
        total = lax.fori_loop(1, NT, lambda j, c: c + zb[j], zb[0])
        xbuf[sp] = total
        for d in range(1, NS):
            remote(xbuf.at[sp], xbuf.at[sp], ar_s.at[n, 1], ar_r.at[n, 1], {"space": at_x(d)}).start()

    def x_total(n, zb, xbuf):
        last = remote(
            xbuf.at[0 : NS - 1], xbuf.at[0 : NS - 1], ar_s.at[n, 1], ar_r.at[n, 1], {"space": at_x(1)}
        )
        last.wait_recv()
        total = xbuf[0]
        for j in range(1, NS):
            total = total + xbuf[j]
        return total

    def reduced_sent(n, zb, xbuf):
        remote(
            zb.at[0 : NT - 1], zb.at[0 : NT - 1], ar_s.at[n, 0], ar_r.at[n, 0], {"tm": at_z(1)}
        ).wait_send()
        remote(
            xbuf.at[0 : NS - 1], xbuf.at[0 : NS - 1], ar_s.at[n, 1], ar_r.at[n, 1], {"space": at_x(1)}
        ).wait_send()

    def halo_copies(n, graw):
        right, left = at_x(1), at_x(NS - 1)
        before = at_z(NT - 1)
        own = pl.ds(0, T)
        later = pl.ds(T, T)
        plan = (
            (graw.at[own, H], graw.at[own, 0], {"space": right}),
            (graw.at[own, 1], graw.at[own, H + 1], {"space": left}),
            (graw.at[own, pl.ds(1, H)], graw.at[later, pl.ds(1, H)], {"tm": before}),
            (graw.at[own, H], graw.at[later, 0], {"tm": before, "space": right}),
            (graw.at[own, 1], graw.at[later, H + 1], {"tm": before, "space": left}),
        )
        return [
            remote(src, dst, halo_s.at[n, i], halo_r.at[n, i], where)
            for i, (src, dst, where) in enumerate(plan)
        ]

    has_right, has_left, has_before, has_after = sp < NS - 1, sp > 0, tm > 0, tm < NT - 1
    sends = (
        has_right,
        has_left,
        has_before,
        jnp.logical_and(has_before, has_right),
        jnp.logical_and(has_before, has_left),
    )
    arrives = (
        has_left,
        has_right,
        has_after,
        jnp.logical_and(has_after, has_left),
        jnp.logical_and(has_after, has_right),
    )

    def halo_start(n, graw):
        for copy, here in zip(halo_copies(n, graw), sends):
            @pl.when(here)
            def _():
                copy.start()

    def halo_wait(n, graw, which):
        copies = halo_copies(n, graw)
        for i in which:
            @pl.when(arrives[i])
            def _():
                copies[i].wait_recv()

    def halo_sent(n, graw):
        for copy, here in zip(halo_copies(n, graw), sends):
            @pl.when(here)
            def _():
                copy.wait_send()

    def feature_copies():
        right, left, after = at_x(1), at_x(NS - 1), at_z(1)
        own, earlier = pl.ds(T, T), pl.ds(0, T)
        w = wide_feat
        plan = (
            (w.at[own, H], w.at[own, 0], {"space": right}),
            (w.at[own, 1], w.at[own, H + 1], {"space": left}),
            (w.at[own, pl.ds(1, H)], w.at[earlier, pl.ds(1, H)], {"tm": after}),
            (w.at[own, H], w.at[earlier, 0], {"tm": after, "space": right}),
            (w.at[own, 1], w.at[earlier, H + 1], {"tm": after, "space": left}),
        )
        return [
            remote(src, dst, halo_s.at[2, i], halo_r.at[2, i], where)
            for i, (src, dst, where) in enumerate(plan)
        ]

    feature_sends = (
        has_right,
        has_left,
        has_after,
        jnp.logical_and(has_after, has_right),
        jnp.logical_and(has_after, has_left),
    )
    feature_arrives = (
        has_left,
        has_right,
        has_before,
        jnp.logical_and(has_before, has_left),
        jnp.logical_and(has_before, has_right),
    )

    def feature_start():
        for copy, here in zip(feature_copies(), feature_sends):
            @pl.when(here)
            def _():
                copy.start()

    def feature_wait():
        for copy, here in zip(feature_copies(), feature_arrives):
            @pl.when(here)
            def _():
                copy.wait_recv()

    def feature_sent():
        for copy, here in zip(feature_copies(), feature_sends):
            @pl.when(here)
            def _():
                copy.wait_send()

    def place_shifted(f, r, values):
        tmp[8 : 8 + W] = values
        for c in range(3):
            ext[f, r, :, c * half : (c + 1) * half] = tmp[9 - c : 9 - c + WP].astype(BF16)

    def shift(graw, first, last):
        @pl.loop(first * (H + 2), last * (H + 2))
        def _(j):
            f, r = j // (H + 2), lax.rem(j, H + 2)
            place_shifted(f, r, graw[f, r].astype(F32))

    def shift_own(graw):
        @pl.loop(0, T * H)
        def _(j):
            place_shifted(j // H, lax.rem(j, H) + 1, graw[j // H, lax.rem(j, H) + 1].astype(F32))

    def shift_edges(graw):
        @pl.loop(0, 2 * T)
        def _(j):
            f, r = j // 2, lax.rem(j, 2) * (H + 1)
            place_shifted(f, r, graw[f, r].astype(F32))

    def taps(f, a, b):
        return ext[f + 2 - a, 2 - b : 2 - b + H].reshape(H * WP, K3)

    def back_part(kernel, f, a, first):
        left = jnp.concatenate([taps(f, a, b) for b in range(3)], axis=1)
        right = jnp.concatenate([kernel[a * 9 + k] for k in range(9)], axis=1)
        product = lax.dot_general(left, right, (((1,), (1,)), ((), ())), preferred_element_type=F32)
        for k in range(2):
            piece = product[:, k * half : (k + 1) * half].reshape(H, WP, half)
            if first:
                acc[k, f * H : (f + 1) * H] = piece
            else:
                acc[k, f * H : (f + 1) * H] += piece

    def exchange(n, f):
        part = pl.ds(f * H, H)
        return remote(
            acc.at[1 - ch, part], acc_in.at[n, part], ch_s.at[n, f], ch_r.at[n, f], {"chan": 1 - ch}
        )

    def lanes(p):
        q, low, high = PIECES[p]
        return q, pl.ds(low * K3, (high - low) * K3)

    def delta_part(p):
        q, low, high = PIECES[p]
        a = 2 - q % 3
        for b in range(low, high):
            if q < 3:
                left = act_t[...]
                right = jnp.concatenate([taps(f, a, b) for f in range(T)], axis=0)
            else:
                left = wide_act_t[b, :, a * H * WP : (a + T) * H * WP]
                right = jnp.concatenate([taps(f, 2, 1) for f in range(T)], axis=0)
            product = lax.dot_general(
                left, right, (((1,), (0,)), ((), ())), preferred_element_type=F32
            )
            xs[q, :, b * K3 : (b + 1) * K3] = product.astype(BF16)
            if q < 3:
                own_f[q, :, b * K3 : (b + 1) * K3] = product

    def chunk(s, part, parts):
        size = R // parts
        return pl.ds(pl.multiple_of(s * R + part * size, size), size)

    def sum_1(p):
        far = at_x(2)
        q, cut = lanes(p)
        return [
            remote(
                xs.at[q, chunk(far, k, 2), cut], xa.at[q, k, :, cut],
                xa_s.at[p, k], xa_r.at[p, k], {"space": at_x(d)},
            )
            for k, d in enumerate((1, NS - 1))
        ]

    def sum_2(p):
        q, cut = lanes(p)
        return [
            remote(
                xs.at[q, chunk(at_x(d), 0, 1), cut], xb.at[q, k, :, cut],
                xb_s.at[p, k], xb_r.at[p, k], {"space": at_x(d)},
            )
            for k, d in enumerate((1, NS - 1))
        ]

    def rs_start(p):
        for copy in sum_1(p):
            copy.start()

    def rs_pass(p):
        q, cut = lanes(p)
        for k, (first, second) in enumerate(zip(sum_1(p), sum_2(p))):
            first.wait_recv()
            rows = chunk(at_x((1, NS - 1)[k]), k, 2)
            xs[q, rows, cut] = (xs[q, rows, cut].astype(F32) + xa[q, k, :, cut].astype(F32)).astype(BF16)
            second.start()

    pairs = NT // 2
    parity = lax.rem(tm, 2)
    place = tm // 2

    def mate(p):
        turned = parity if p % 2 == 0 else 1 - parity
        return {"tm": lax.rem(tm + 1 - 2 * turned + NT, NT)}

    def to_mate(p):
        q, cut = lanes(p)
        return remote(
            zs.at[q, 1 - parity, :, :, cut], za.at[q, :, :, cut], za_s.at[p], za_r.at[p], mate(p)
        )

    def rs_z1(p):
        q, cut = lanes(p)
        for copy in sum_2(p):
            copy.wait_recv()
        kept = xs[q, chunk(sp, 0, 1), cut].astype(F32)
        zf[:, cut] = kept + xb[q, 0, :, cut].astype(F32) + xb[q, 1, :, cut].astype(F32)
        for t in range(NT):
            rows = zf[t * share : (t + 1) * share, cut]
            zk[q, t % 2, t // 2, :, cut] = rows
            zs[q, t % 2, t // 2, :, cut] = rows.astype(BF16)
        to_mate(p).start()

    def rs_z2(p):
        q, cut = lanes(p)
        to_mate(p).wait_recv()

        @pl.loop(0, pairs)
        def _(j):
            both = zk[q, parity, j, :, cut] + za[q, j, :, cut].astype(F32)
            zk[q, parity, j, :, cut] = both
            zc[q, j, :, cut] = both.astype(BF16)

        @pl.loop(1, pairs)
        def _(k):
            d = lax.rem(k + pairs // 2 - 1, pairs - 1) + 1
            to = lax.rem(place + d, pairs)
            remote(
                zc.at[q, to, :, cut], zr.at[q, d - 1, :, cut], z_s.at[p], z_r.at[p],
                {"tm": 2 * to + parity},
            ).start()

    def z_all(p):
        q, cut = lanes(p)
        return remote(
            zc.at[q, pl.ds(0, pairs - 1), :, cut], zr.at[q, :, :, cut], z_s.at[p], z_r.at[p], mate(p)
        )

    def rs_end(p):
        q, low, high = PIECES[p]
        cut = lanes(p)[1]
        z_all(p).wait_recv()
        total = zk[q, parity, place, :, cut]
        for j in range(pairs - 1):
            total = total + zr[q, j, :, cut].astype(F32)
        out, a = (d2, d1)[q // 3], 2 - q % 3
        for k in range(3 * (high - low)):
            out[a * 9 + 3 * low + k] = total[:, k * half : (k + 1) * half]

    def rs_sent(p):
        for copy in sum_1(p) + sum_2(p):
            copy.wait_send()
        to_mate(p).wait_send()
        z_all(p).wait_send()

    steps = (NT // 2, NT - 1 - NT // 2)
    band = NS * share

    def band_of(t):
        return pl.ds(pl.multiple_of(t * band, band), band)

    def hop(q, way, k):
        if way == 0:
            dest, to, slot = at_z(steps[0] - k), at_z(1), k
        else:
            dest, to, slot = at_z(NT - steps[1] + k), at_z(NT - 1), steps[0] + k
        return dest, remote(
            xs.at[q, band_of(dest)], ring.at[q, slot], hop_s.at[q, slot], hop_r.at[q, slot], {"tm": to}
        )

    def tick(q, way, k):
        dest, copy = hop(q, way, k)
        if k > 0:
            hop(q, way, k - 1)[1].wait_recv()
            came = ring[q, way * steps[0] + k - 1].astype(F32)
            xs[q, band_of(dest)] = (own_f[q, band_of(dest)] + came).astype(BF16)
        copy.start()

    def ticks(way, k):
        for q in range(3):
            tick(q, way, k)

    def across(q, d):
        return remote(
            ring_s.at[q, at_x(d)], ring_r.at[q, d - 1], last_s.at[q, d - 1], last_r.at[q, d - 1],
            {"space": at_x(d)},
        )

    def ring_pass(q):
        for way in range(2):
            hop(q, way, steps[way] - 1)[1].wait_recv()
        total = own_f[q, band_of(tm)]
        total = total + ring[q, steps[0] - 1].astype(F32) + ring[q, NT - 2].astype(F32)
        zf[0:band] = total
        for x in range(NS):
            rows = zf[x * share : (x + 1) * share]
            ring_k[q, x] = rows
            ring_s[q, x] = rows.astype(BF16)
        for d in range(1, NS):
            across(q, d).start()

    def ring_end(q):
        total = ring_k[q, sp]
        for d in range(1, NS):
            across(q, d).wait_recv()
            total = total + ring_r[q, d - 1].astype(F32)
        for k in range(9):
            d2[(2 - q) * 9 + k] = total[:, k * half : (k + 1) * half]

    def ring_sent(q):
        for way in range(2):
            for k in range(steps[way]):
                hop(q, way, k)[1].wait_send()
        for d in range(1, NS):
            across(q, d).wait_send()

    def activated(x, n):
        scaled = (x.astype(F32) - stats[2 * n : 2 * n + 1]) * stats[2 * n + 1 : 2 * n + 2]
        scaled = scaled * gains[n : n + 1]
        return scaled * jax.nn.sigmoid(scaled)

    def turned(order, cells):
        return lax.dot_general(
            order, cells, (((1,), (1,)), ((), ())), preferred_element_type=F32
        ).astype(BF16)

    def activate_hidden():
        @pl.loop(0, T * H)
        def _(j):
            t, h = row_of(j)
            act[j, 0:W] = activated(hid[t, h], 1).astype(BF16)

        order = jnp.where(same, 1.0, 0.0).astype(BF16)
        act_t[...] = turned(order, act[...].reshape(T * H * WP, C))

    def activate_features():
        @pl.loop(0, 2 * T * (H + 2))
        def _(j):
            f, r = j // (H + 2), lax.rem(j, H + 2)
            inside = jnp.logical_and(
                jnp.logical_and(jnp.logical_or(r > 0, has_left), jnp.logical_or(r < H + 1, has_right)),
                jnp.logical_or(f >= T, has_before),
            )
            value = activated(wide_feat[f, r], 0)
            wide_act[f, r, 0:W] = jnp.where(inside, value, 0.0).astype(BF16)

        for b in range(3):
            cells = wide_act[:, b : b + H].reshape(2 * T * H * WP, C)
            wide_act_t[b] = turned(perm[...], cells)

    def own_row(ref, k):
        return ref[k : k + 1, pl.ds(off, half)]

    def centred_row(ref, n, t, h):
        x = ref[t, h, :, pl.ds(off, half)].astype(F32)
        return (x - own_row(stats, 2 * n)) * own_row(stats, 2 * n + 1)

    def slopes(ref, n):
        exchanged = 1 - n

        def row(j, carry):
            t, h = row_of(j)
            centred = centred_row(ref, n, t, h)
            scaled = centred * own_row(gains, n)
            gate = jax.nn.sigmoid(scaled)
            upstream = acc[ch, j, 0:W] + acc_in[exchanged, j, 0:W]
            value = upstream * gate * (1.0 + scaled * (1.0 - gate))
            slope[j, 0:W] = value
            return (
                carry[0] + jnp.sum(value, axis=0, keepdims=True),
                carry[1] + jnp.sum(value * centred, axis=0, keepdims=True),
            )

        zero = jnp.zeros((1, half), F32)
        return lax.fori_loop(0, T * H, row, (zero, zero))

    def norm_terms(n, totals):
        both = group_sum(totals * own_row(gains, n), half) * (1.0 / members)
        gg[n : n + 1] = totals[1:2]
        return both[0:1], both[1:2]

    def grad_row(ref, n, t, h, terms):
        first, second = terms
        centred = centred_row(ref, n, t, h)
        inner = slope[t * H + h, 0:W] * own_row(gains, n) - first - centred * second
        return own_row(stats, 2 * n + 1) * inner

    def hidden_rows(totals):
        terms = norm_terms(1, totals)

        @pl.loop(0, T * H)
        def _(j):
            t, h = row_of(j)
            graw1[t, h + 1] = grad_row(hid, 1, t, h, terms).astype(BF16)

    def feature_rows(totals):
        terms = norm_terms(0, totals)

        @pl.loop(0, T)
        def _(t):
            for h in range(H):
                base = graw2[t, h + 1].astype(F32)
                turn_half[t, :, h, :] = base + grad_row(feat, 0, t, h, terms)
            fgrad[t] = turn_half[t].astype(BF16)

    def by_rows(source, target):
        @pl.loop(0, T)
        def _(t):
            turn[...] = source[t].astype(F32)
            for h in range(H):
                target[t, h] = turn[:, h, :].astype(BF16)

    def reduce_slopes(n, parts):
        for k in range(2):
            zb_b[n, tm, k : k + 1] = parts[k]
        along_z(2 - n, zb_b.at[n])

    along_z(0, zb_a)
    halo_start(0, graw2)
    tmp[...] = jnp.zeros_like(tmp)
    act[...] = jnp.zeros_like(act)
    wide_act[...] = jnp.zeros_like(wide_act)
    for graw in (graw2, graw1):
        @pl.when(sp == 0)
        def _():
            graw[:, 0] = jnp.zeros((2 * T, W, half), BF16)

        @pl.when(sp == NS - 1)
        def _():
            graw[:, H + 1] = jnp.zeros((2 * T, W, half), BF16)

        @pl.when(tm == NT - 1)
        def _():
            graw[T : 2 * T] = jnp.zeros((T, H + 2, W, half), BF16)

    rows = lax.broadcasted_iota(jnp.int32, (C, C), 0)
    cols = lax.broadcasted_iota(jnp.int32, (C, C), 1)
    within = lax.rem(rows, R)
    source = within // share * (NS * share) + rows // R * share + lax.rem(within, share)
    perm[...] = jnp.where(cols == source, 1.0, 0.0).astype(BF16)
    same = rows == cols
    block_sum[...] = jnp.where(rows // per == cols // per, 1.0, 0.0).astype(F32)
    by_rows(feat_n, feat)
    feature_start()
    by_rows(hid_n, hid)

    def back_parts(kernel, later, n=None):
        for f in range(T):
            for a in (2, 1, 0):
                if (f + 2 - a >= T) == later:
                    back_part(kernel, f, a, a == 2)
            if later:
                exchange(n, f).start()

    halo_wait(0, graw2, (0, 1))
    shift(graw2, 0, T)
    loads[3].wait()
    back_parts(k2, False)
    z_to_x(0, zb_a, xb_a)
    halo_wait(0, graw2, (2, 3, 4))
    shift(graw2, T, 2 * T)
    back_parts(k2, True, 0)
    totals = lax.dot_general(
        x_total(0, zb_a, xb_a), spread_sum[...], (((1,), (1,)), ((), ())),
        precision=lax.Precision.HIGHEST, preferred_element_type=F32,
    ) * (1.0 / members)
    for n in range(2):
        mean = totals[2 * n : 2 * n + 1]
        spread = totals[2 * n + 1 : 2 * n + 2] - mean * mean
        stats[2 * n : 2 * n + 1] = mean
        stats[2 * n + 1 : 2 * n + 2] = lax.rsqrt(spread + EPS)
    for f in range(T):
        exchange(0, f).wait_recv()
    reduce_slopes(1, slopes(hid, 1))
    activate_hidden()
    for p in range(3):
        delta_part(p)
        tick(p, 0, 0)
        tick(p, 1, 0)
    feature_wait()
    activate_features()
    z_to_x(1, zb_b.at[1], xb_b.at[1])
    ticks(0, 1)
    ticks(1, 1)
    totals_two = x_total(1, zb_b.at[1], xb_b.at[1])

    hidden_rows(totals_two)
    halo_start(1, graw1)
    shift_own(graw1)
    for p in range(3, 8):
        delta_part(p)
        rs_start(p)
        if p == 3:
            ticks(0, 2)
            ticks(1, 2)
    loads[4].wait()
    for f in range(T):
        exchange(0, f).wait_send()
    halo_wait(1, graw1, (0, 1))
    shift_edges(graw1)
    ticks(0, 3)
    back_parts(k1, False)
    for p in range(3, 8):
        rs_pass(p)
    halo_wait(1, graw1, (2, 3, 4))
    ticks(0, 4)
    shift(graw1, T, 2 * T)
    back_parts(k1, True, 1)
    ticks(1, 3)
    ticks(0, 5)
    rs_z1(3)
    for f in range(T):
        exchange(1, f).wait_recv()
    reduce_slopes(0, slopes(feat, 0))
    ticks(1, 4)
    ticks(0, 6)
    rs_z1(4)
    rs_z2(3)
    ticks(1, 5)
    for p in range(5, 8):
        rs_z1(p)
    ticks(0, 7)
    rs_z2(4)
    z_to_x(2, zb_b.at[0], xb_b.at[0])
    ticks(1, 6)
    for p in range(5, 8):
        rs_z2(p)
    feature_rows(x_total(2, zb_b.at[0], xb_b.at[0]))
    for q in range(3):
        ring_pass(q)
    for p in range(3, 8):
        rs_end(p)
    for q in range(3):
        ring_end(q)

    halo_sent(0, graw2)
    halo_sent(1, graw1)
    feature_sent()
    reduced_sent(0, zb_a, xb_a)
    reduced_sent(1, zb_b.at[1], xb_b.at[1])
    reduced_sent(2, zb_b.at[0], xb_b.at[0])
    for f in range(T):
        exchange(1, f).wait_send()
    for p in range(3, 8):
        rs_sent(p)
    for q in range(3):
        ring_sent(q)


def hand_on(*refs):
    count = len(refs) // 2
    for source, target in zip(refs[:count], refs[count:]):
        target[...] = source[...]


def shards(features, hidden, cotangent, kernel_one, kernel_two, gains):
    T, H, W, C = features.shape
    half = kernel_one.shape[4]
    NT, NS = lax.axis_size("tm"), lax.axis_size("space")
    share = C // (NT * NS)
    R = NT * share
    WP = padded_width(W)
    wide = 9 * half

    def by_tap(kernel):
        return jnp.transpose(kernel, (1, 2, 3, 0, 4)).reshape(27, C, half)

    vmem = pl.BlockSpec(memory_space=pltpu.VMEM)
    hbm = pl.BlockSpec(memory_space=pl.ANY)
    DMA = pltpu.SemaphoreType.DMA
    call = pl.pallas_call(
        functools.partial(body, (T, H, W, C, half, NT, NS)),
        out_shape=(
            jax.ShapeDtypeStruct((T, W, H, half), BF16),
            jax.ShapeDtypeStruct((27, share, half), F32),
            jax.ShapeDtypeStruct((27, share, half), F32),
            jax.ShapeDtypeStruct((2, half), F32),
        ),
        in_specs=[hbm] * 5 + [vmem],
        out_specs=(vmem,) * 4,
        scratch_shapes=[
            pltpu.VMEM((T, W, H, C), BF16),
            pltpu.VMEM((T, W, H, C), BF16),
            pltpu.VMEM((T, W, H, C), BF16),
            pltpu.VMEM((2 * T, H + 2, W, C), BF16),
            pltpu.VMEM((T, H, W, C), BF16),
            pltpu.VMEM((27, C, half), BF16),
            pltpu.VMEM((27, C, half), BF16),
            pltpu.VMEM((2 * T, H + 2, W, half), BF16),
            pltpu.VMEM((2 * T, H + 2, W, half), BF16),
            pltpu.VMEM((W, H, C), F32),
            pltpu.VMEM((T, W, H, half), F32),
            pltpu.VMEM((WP + 16, half), F32),
            pltpu.VMEM((2 * T, H + 2, WP, 3 * half), BF16),
            pltpu.VMEM((T * H, WP, C), BF16),
            pltpu.VMEM((C, T * H * WP), BF16),
            pltpu.VMEM((2 * T, H + 2, WP, C), BF16),
            pltpu.VMEM((3, C, 2 * T * H * WP), BF16),
            pltpu.VMEM((3, C, wide), F32),
            pltpu.VMEM((C, C), BF16),
            pltpu.VMEM((C, C), F32),
            pltpu.VMEM((C, half), F32),
            pltpu.VMEM((2, T * H, WP, half), F32),
            pltpu.VMEM((2, T * H, WP, half), F32),
            pltpu.VMEM((T * H, WP, half), F32),
            pltpu.VMEM((8, C), F32),
            pltpu.VMEM((NT, 4, half), F32),
            pltpu.VMEM((NS, 4, half), F32),
            pltpu.VMEM((2, NT, 2, half), F32),
            pltpu.VMEM((2, NS, 2, half), F32),
            pltpu.VMEM((6, C, wide), BF16),
            pltpu.VMEM((6, 2, R // 2, wide), BF16),
            pltpu.VMEM((6, 2, R, wide), BF16),
            pltpu.VMEM((R, wide), F32),
            pltpu.VMEM((6, 2, NT // 2, share, wide), F32),
            pltpu.VMEM((6, 2, NT // 2, share, wide), BF16),
            pltpu.VMEM((6, NT // 2, share, wide), BF16),
            pltpu.VMEM((6, NT // 2, share, wide), BF16),
            pltpu.VMEM((6, NT // 2 - 1, share, wide), BF16),
            pltpu.VMEM((3, NT - 1, NS * share, wide), BF16),
            pltpu.VMEM((3, NS, share, wide), F32),
            pltpu.VMEM((3, NS, share, wide), BF16),
            pltpu.VMEM((3, NS - 1, share, wide), BF16),
            DMA((5,)),
            DMA((3, 5)),
            DMA((3, 5)),
            DMA((3, 2)),
            DMA((3, 2)),
            DMA((2, T)),
            DMA((2, T)),
            DMA((8, 2)),
            DMA((8, 2)),
            DMA((8, 2)),
            DMA((8, 2)),
            DMA((8,)),
            DMA((8,)),
            DMA((8,)),
            DMA((8,)),
            DMA((3, NT - 1)),
            DMA((3, NT - 1)),
            DMA((3, NS - 1)),
            DMA((3, NS - 1)),
        ],
        compiler_params=pltpu.CompilerParams(
            collective_id=0, has_side_effects=True, vmem_limit_bytes=60 * 1024 * 1024
        ),
        name="block_back",
    )
    def by_column(field):
        return jnp.transpose(field, (0, 2, 1, 3))

    made = call(
        by_column(features), by_column(hidden), by_column(cotangent),
        by_tap(kernel_one), by_tap(kernel_two), gains,
    )
    fgrad, d1, d2, gg = pl.pallas_call(
        hand_on,
        out_shape=tuple(jax.ShapeDtypeStruct(x.shape, x.dtype) for x in made),
        in_specs=[vmem] * 4,
        out_specs=(vmem,) * 4,
        name="hand_on",
    )(*made)

    def by_channel(delta):
        return jnp.transpose(delta.reshape(3, 3, 3, share, half), (3, 0, 1, 2, 4))

    return (by_column(fgrad), by_channel(d1), by_channel(d2), gg)


def solution(mesh):
    placed = (
        P(("clip", "tm"), "space", None, None),
        P(("clip", "tm"), "space", None, None),
        P(("clip", "tm"), "space", None, None),
        P(None, None, None, None, "chan"),
        P(None, None, None, None, "chan"),
        P(),
    )
    return jax.shard_map(
        shards,
        mesh=mesh,
        in_specs=placed,
        out_specs=(
            P(("clip", "tm"), "space", None, "chan"),
            P(("clip", "tm", "space"), None, None, None, "chan"),
            P(("clip", "tm", "space"), None, None, None, "chan"),
            P("clip", "chan"),
        ),
        check_vma=False,
    )
```
